512 devices in a mesh: dp: 64 (over y, z), mp: 8 (over x, core).
Axes of the slice: x: 4, y: 4, z: 16, core: 2. Of those that a mesh axis runs over, the one named last changes fastest.
Arguments:
- tokens: bfloat16 [512, 8192], P('mp', 'dp'), may hold values from -6 to 6
- norm_gain: float32 [8192], replicated, may hold values from 0.25 to 1.75
- query_weight: bfloat16 [8192, 8192], P(None, 'dp'), may hold values from -0.0625 to 0.0625
- out_weight: bfloat16 [8192, 8192], P(None, 'dp'), may hold values from -0.0625 to 0.0625
- gate_scalar: float32 [1], replicated, may hold values from 0.4 to 1.5
- image_keys: bfloat16 [128, 64, 8192], P('mp', None, 'dp'), may hold values from -260 to 260
- image_values: bfloat16 [128, 64, 8192], P('mp', None, 'dp'), may hold values from -6 to 6
- active_image: int32 [128, 4], replicated, may hold values from 0 to 127
- image_slot: int32 [128], replicated, may hold values from 0 to 127, each once
Outputs:
- mixed: bfloat16 [512, 8192], P('mp', 'dp')
The draws below stay inside these ranges and needn't reach their ends.
Inputs may be any that keep to these rules, and one draw needn't show every extreme that they name: `image_slot`: each slot 0 to 127 once.
All inputs are finite; a program needn't handle non-finite values.
Results may differ from the reference program's by a relative error of at most 0.0047.
Values may be sent and summed in bfloat16 or wider, within the bound.
A program may use at most 64 MiB of HBM per device.

```python
import math
import jax
import jax.numpy as jnp
import numpy as np
from jax import lax

D = 8192
DH = 128
VT = 64
STEPS = 4
HEADS = 64
SEQS = 128
ROWS = 512
IMAGES = 128


def draw_image_keys(key, part):
    first = jax.random.fold_in(jax.random.fold_in(key, 17), 0)
    shape = (IMAGES, VT, HEADS * DH)
    return jax.random.normal(first, shape, jnp.float32).astype(jnp.bfloat16)


def plant(drawn, key, smallest, top_value):
    place = [jax.random.randint(jax.random.fold_in(key, axis), (), 0, length) for axis, length in enumerate(drawn.shape)]
    widest = drawn.shape.index(max(drawn.shape))
    next_to = place[:widest] + [(place[widest] + 1) % drawn.shape[widest]] + place[widest + 1:]
    return drawn.at[tuple(place)].set(smallest).at[tuple(next_to)].set(top_value)


def levels(own_key, extent, cuts, least, high):
    loudness = 1.0
    for dim, parts in cuts:
        steps = jax.random.uniform(jax.random.fold_in(jax.random.fold_in(own_key, 6), dim), (parts,), jnp.float32, least / len(cuts), high / len(cuts))
        loudness = loudness * jnp.repeat(jnp.exp(steps), extent[dim] // parts).reshape((-1,) + (1,) * (len(extent) - 1 - dim))
    return loudness


def rank_table(count, skew):
    loads = [(1 << 20) // math.isqrt(grade ** skew) + 1 for grade in range(1, count + 1)]
    deviation = 1 + sum(loads) // (1 << 30)
    return np.cumsum(np.array([max(1, weight // deviation) for weight in loads]))


def ranked(rng, shape, count, skew):
    grid = rank_table(count, skew)
    pick = jax.random.randint(jax.random.fold_in(rng, 1), shape, 0, int(grid[count - 1]))
    rank = jnp.searchsorted(jnp.asarray(grid, jnp.int32), pick, side="right")
    return jax.random.permutation(jax.random.fold_in(rng, 2), count)[rank].astype(jnp.int32)


def normal_values(rng, shape, deviation, reach, shards=(), held_as=jnp.bfloat16):
    level = levels(rng, shape, shards, -0.22, 0.18) if shards else 1.0
    drawn = jax.random.normal(rng, shape, jnp.float32) * deviation * level
    return jnp.minimum(jnp.maximum(drawn, -reach), reach).astype(held_as)


def setup_inputs(seed: int = 0) -> dict:
    keys = jax.random.split(jax.random.key(seed), 10)
    return {
        "tokens": normal_values(keys[0], (ROWS, D), 1.0, 6.0, ((0, 8), (1, 64))),
        "norm_gain": jnp.clip(1.0 + 0.15 * jax.random.normal(keys[1], (D,), jnp.float32), 0.25, 1.75),
        "query_weight": normal_values(keys[2], (D, HEADS * DH), D ** -0.5, 0.0625, ((1, 64),)),
        "out_weight": normal_values(keys[3], (HEADS * DH, D), (HEADS * DH) ** -0.5, 0.0625, ((1, 64),)),
        "gate_scalar": jnp.clip(jax.random.uniform(keys[4], (1,), jnp.float32, 0.4, 1.5), 0.4, 1.5),
        "image_keys": draw_image_keys(jax.random.fold_in(keys[9], 71), 0),
        "image_values": normal_values(keys[6], (IMAGES, VT, HEADS * DH), 1.0, 6.0, ((0, 8), (2, 64))),
        "active_image": plant(ranked(keys[7], (SEQS, STEPS), IMAGES, 2), jax.random.fold_in(keys[7], 3), 0, IMAGES - 1).astype(jnp.int32),
        "image_slot": jax.random.permutation(keys[8], IMAGES).astype(jnp.int32),
    }


epsilon = 1e-05

def reference(tokens, norm_gain, query_weight, out_weight, gate_scalar, image_keys, image_values, active_image, image_slot):
    widened = tokens.astype(jnp.float32)
    average = lax.optimization_barrier(jnp.mean(widened, axis=1, keepdims=True))
    centred = widened - average
    variance = lax.optimization_barrier(jnp.mean(centred * centred, axis=1, keepdims=True))
    normed = (centred * lax.rsqrt(variance + epsilon) * norm_gain).astype(jnp.bfloat16)
    queries = jnp.dot(normed, query_weight, preferred_element_type=jnp.float32).astype(jnp.bfloat16)
    wanted = image_slot[active_image.reshape(-1)]

    def one_head(head_index):
        offset = head_index * DH
        head_queries = lax.dynamic_slice_in_dim(queries, offset, DH, 1).astype(jnp.float32)
        head_keys = lax.dynamic_slice_in_dim(image_keys, offset, DH, 2)[wanted].astype(jnp.float32)
        head_values = lax.dynamic_slice_in_dim(image_values, offset, DH, 2)[wanted].astype(jnp.float32)
        scores = jnp.einsum('rd,rtd->rt', head_queries, head_keys) * DH ** (-0.5)
        largest = lax.optimization_barrier(jnp.max(scores, axis=1, keepdims=True))
        expo = jnp.exp(scores - largest)
        totals = lax.optimization_barrier(jnp.sum(expo, axis=1, keepdims=True))
        rounded = lax.optimization_barrier((expo / totals).astype(jnp.bfloat16))
        return jnp.einsum('rt,rtd->rd', rounded.astype(jnp.float32), head_values)
    outputs = lax.map(one_head, jnp.arange(HEADS, dtype=jnp.int32))
    attended = jnp.transpose(outputs, (1, 0, 2)).reshape(ROWS, HEADS * DH).astype(jnp.bfloat16)
    projected = jnp.dot(attended, out_weight, preferred_element_type=jnp.float32)
    return (widened + jnp.tanh(gate_scalar[0]) * projected).astype(jnp.bfloat16)
```

```python
import jax
import jax.numpy as jnp
from jax import lax
from jax.experimental import pallas as pl
from jax.experimental.pallas import tpu as pltpu
from jax.sharding import PartitionSpec as P

MESH = pl.DeviceIdType.MESH
NY, NZ, NX = 4, 16, 4
ND = NY * NZ
ROWS = 64
DH = 128
VT = 64
OWN = 16
IMAGES = 128
HALF = ROWS // 2
EPS = 1e-05
F32 = jnp.float32
BF16 = jnp.bfloat16


def kernel(
    tok_h, gain_h, wq_h, wo_h, gate_s, key_h, val_h, act_s, slot_s,
    out_ref,
    tbuf, abuf, wq, wo, gain, kbuf, vbuf, qf, of,
    local_sem, t_send, t_recv, a_send, a_recv, kv_send, kv_recv,
):
    dp = lax.axis_index("dp")
    mp = lax.axis_index("mp")
    y, z = dp // NZ, lax.rem(dp, NZ)
    x, core = mp // 2, lax.rem(mp, 2)
    ys = [lax.rem(y + d, NY) for d in range(NY)]
    zs = [lax.rem(z + d, NZ) for d in range(NZ)]
    xs = [lax.rem(x + d, NX) for d in range(NX)]

    def block(dy, dz):
        return ys[dy % NY] * NZ + zs[dz % NZ]

    def plane_peer(py, pz):
        return (block(py, pz), mp)

    def line_peer(px):
        return (dp, xs[px % NX] * 2 + core)

    sibling = (dp, x * 2 + (1 - core))

    locals_ = [
        pltpu.make_async_copy(tok_h, tbuf.at[dp], local_sem.at[0]),
        pltpu.make_async_copy(gain_h, gain, local_sem.at[1]),
        pltpu.make_async_copy(wq_h, wq, local_sem.at[2]),
        pltpu.make_async_copy(wo_h, wo, local_sem.at[3]),
        pltpu.make_async_copy(key_h, kbuf.at[pl.ds(mp * OWN, OWN)], local_sem.at[4]),
        pltpu.make_async_copy(val_h, vbuf.at[pl.ds(mp * OWN, OWN)], local_sem.at[5]),
    ]
    for copy in locals_:
        copy.start()

    barrier = pltpu.get_barrier_semaphore()
    partners = [plane_peer(0, d) for d in (1, -1, 2, -2, 5, -5)]
    partners += [plane_peer(d, 0) for d in (1, -1)]
    partners += [line_peer(1), line_peer(-1), sibling]
    for peer in partners:
        pl.semaphore_signal(barrier, inc=1, device_id=peer, device_id_type=MESH)
    pl.semaphore_wait(barrier, len(partners))

    kv = ((kbuf, key_h, 0), (vbuf, val_h, 1))

    def images(px, same, part=None):
        owner = xs[px % NX] * 2 + (core if same else 1 - core)
        first, count = owner * OWN, OWN
        if part is not None:
            count = OWN // 2
            first = first + part * count
        return pl.ds(pl.multiple_of(first, count), count)

    def kv_copy(which, source, where, peer, sem):
        buf, _, n = kv[which]
        return pltpu.make_async_remote_copy(
            src_ref=source, dst_ref=buf.at[where], send_sem=kv_send.at[n],
            recv_sem=kv_recv.at[n, sem], device_id=peer, device_id_type=MESH)

    def kv_own(which):
        source = kv[which][1]
        where = images(0, True)
        kv_copy(which, source, where, line_peer(1), 0).start()
        kv_copy(which, source, where, line_peer(-1), 1).start()
        kv_copy(which, source, where, sibling, 4).start()

    def kv_wait(which, where, sem):
        buf = kv[which][0]
        kv_copy(which, buf.at[where], where, sibling, sem).wait_recv()

    def kv_pass(which):
        buf = kv[which][0]
        for px, sem, part in ((-1, 0, 0), (1, 1, 1)):
            where = images(px, True)
            kv_wait(which, where, sem)
            half = images(px, True, part)
            kv_copy(which, buf.at[half], half, line_peer(-px), 2 + part).start()
            kv_copy(which, buf.at[where], where, sibling, 5 + sem).start()

    def kv_pass_half(which):
        buf = kv[which][0]
        for part in (0, 1):
            half = images(2, True, part)
            kv_wait(which, half, 2 + part)
            kv_copy(which, buf.at[half], half, sibling, 7 + part).start()

    def kv_finish(which):
        kv_wait(which, images(0, False), 4)
        kv_wait(which, images(-1, False), 5)
        kv_wait(which, images(1, False), 6)
        kv_wait(which, images(2, False, 0), 7)
        kv_wait(which, images(2, False, 1), 8)

    def gather(buf, send_sem, recv_sem):
        def copy(dy, dz, py, pz, part=None):
            place = buf.at[block(dy, dz)]
            sem = ((dy - py) % NY) * NZ + (dz - pz) % NZ
            if part is not None:
                place = place.at[pl.ds(part * HALF, HALF)]
                sem = sem if part == 0 else ND
            return pltpu.make_async_remote_copy(
                src_ref=place, dst_ref=place, send_sem=send_sem,
                recv_sem=recv_sem.at[sem], device_id=plane_peer(py, pz), device_id_type=MESH)

        def wait(dy, dz):
            if dy % NY == 0 and dz % NZ == 8:
                copy(0, 7, 0, -1, 0).wait_recv()
                part = buf.at[block(0, 8)].at[pl.ds(HALF, HALF)]
                pltpu.make_async_remote_copy(
                    src_ref=part, dst_ref=part, send_sem=send_sem, recv_sem=recv_sem.at[ND],
                    device_id=plane_peer(0, 1), device_id_type=MESH).wait_recv()
                return
            place = buf.at[block(dy, dz)]
            pltpu.make_async_remote_copy(
                src_ref=place, dst_ref=place, send_sem=send_sem,
                recv_sem=recv_sem.at[(dy % NY) * NZ + dz % NZ],
                device_id=plane_peer(0, 1), device_id_type=MESH).wait_recv()

        def along_y(dz):
            copy(0, dz, 1, 0).start()
            copy(0, dz, -1, 0).start()

        def own():
            for pz in (5, -5, 1, -1, 2, -2):
                copy(0, 0, 0, pz).start()
            along_y(0)

        def line(*offsets):
            for dz in offsets:
                wait(0, dz)
                if dz in (5, -5):
                    for pz in (1, -1, 2, -2):
                        copy(0, dz, 0, pz).start()
                if dz == 7:
                    copy(0, dz, 0, -1, 0).start()
                if dz == -7:
                    copy(0, dz, 0, 1, 1).start()
                along_y(dz)

        def relay(*offsets):
            for dz in offsets:
                for dy in (1, -1):
                    wait(dy, dz)
                    if (dz % 2 == 0) == (dy == 1):
                        copy(dy, dz, -dy, 0).start()

        def last():
            for dz in range(NZ):
                wait(2, dz)

        def sent():
            whole = buf.at[pl.ds(0, ND - 1)]
            pltpu.make_async_copy(whole, whole, send_sem).wait()

        return own, line, relay, last, sent

    own, line, relay, last, t_sent = gather(tbuf, t_send.at[0], t_recv)
    locals_[0].wait()
    own()
    kv_own(0)
    kv_own(1)
    line(1, -1)
    relay(0)
    line(2, -2)
    relay(1, -1)
    line(5, -5)
    relay(2, -2)
    line(4, -4, 6, -6)
    relay(5, -5)
    line(3, -3, 7, -7)
    kv_pass(0)
    relay(4, -4, 6, -6)
    line(8)
    relay(3, -3, 7, -7)
    relay(8)
    kv_pass(1)
    last()

    def add_row(d, total):
        return total + tbuf[d].astype(F32)

    total = lax.fori_loop(0, ND, add_row, jnp.zeros((ROWS, DH), F32), unroll=8)
    mean = jnp.sum(total, axis=1, keepdims=True) * (1.0 / (ND * DH))
    mean_b = jnp.broadcast_to(mean, (ROWS, DH))

    def add_square(d, total):
        c = tbuf[d].astype(F32) - mean_b
        return total + c * c

    square = lax.fori_loop(0, ND, add_square, jnp.zeros((ROWS, DH), F32), unroll=8)
    variance = jnp.sum(square, axis=1, keepdims=True) * (1.0 / (ND * DH))
    scale_b = jnp.broadcast_to(lax.rsqrt(variance + EPS), (ROWS, DH))
    locals_[1].wait()
    locals_[2].wait()

    def project(i, acc):
        parts = []
        for j in range(4):
            d = i * 4 + j
            g = gain[pl.ds(d, 1), :]
            parts.append((((tbuf[d].astype(F32) - mean_b) * scale_b) * g).astype(BF16))
        lhs = jnp.concatenate(parts, axis=1)
        rhs = wq[pl.ds(pl.multiple_of(i * 4 * DH, 4 * DH), 4 * DH), :]
        return acc + jnp.dot(lhs, rhs, preferred_element_type=F32)

    queries = lax.fori_loop(0, ND // 4, project, jnp.zeros((ROWS, DH), F32), unroll=4)
    qf[...] = queries.astype(BF16).astype(F32)

    kv_pass_half(0)
    kv_pass_half(1)
    locals_[4].wait()
    locals_[5].wait()
    kv_finish(0)
    kv_finish(1)

    def attend(i, carry):
        outs = []
        for j in range(8):
            image = act_s[j % 4, mp * (ROWS // 4) + i * 2 + j // 4]
            slot = slot_s[image]
            q = qf[pl.ds(i * 8 + j, 1), :]
            s = jnp.sum(kbuf[slot].astype(F32) * q, axis=1, keepdims=True) * (DH ** -0.5)
            e = jnp.exp(s - jnp.max(s, axis=0, keepdims=True))
            p = (e / jnp.sum(e, axis=0, keepdims=True)).astype(BF16).astype(F32)
            outs.append(jnp.sum(p * vbuf[slot].astype(F32), axis=0, keepdims=True))
        of[pl.ds(pl.multiple_of(i * 8, 8), 8), :] = jnp.concatenate(outs, axis=0)
        return carry

    lax.fori_loop(0, ROWS // 8, attend, 0)
    abuf[dp] = of[...].astype(BF16)

    own, line, relay, last, a_sent = gather(abuf, a_send.at[0], a_recv)
    own()
    line(1, -1)
    relay(0)
    line(2, -2)
    relay(1, -1)
    line(5, -5)
    relay(2, -2)
    line(4, -4, 6, -6)
    relay(5, -5)
    line(3, -3, 7, -7)
    relay(4, -4, 6, -6)
    line(8)
    relay(3, -3, 7, -7)
    relay(8)
    last()

    locals_[3].wait()

    def project_out(i, acc):
        lhs = jnp.concatenate([abuf[i * 4 + j] for j in range(4)], axis=1)
        rhs = wo[pl.ds(pl.multiple_of(i * 4 * DH, 4 * DH), 4 * DH), :]
        return acc + jnp.dot(lhs, rhs, preferred_element_type=F32)

    projected = lax.fori_loop(0, ND // 4, project_out, jnp.zeros((ROWS, DH), F32), unroll=4)
    gate = jnp.tanh(jnp.full((ROWS, DH), gate_s[0], F32))
    out_ref[...] = (tbuf[dp].astype(F32) + gate * projected).astype(BF16)

    t_sent()
    a_sent()
    for which in (0, 1):
        whole = kv[which][0].at[pl.ds(0, 7 * OWN)]
        pltpu.make_async_copy(whole, whole, kv_send.at[which]).wait()


def body(tokens, norm_gain, query_weight, out_weight, gate_scalar, image_keys, image_values, active_image, image_slot):
    hbm = pl.BlockSpec(memory_space=pltpu.HBM)
    smem = pl.BlockSpec(memory_space=pltpu.SMEM)
    vmem = pl.BlockSpec(memory_space=pltpu.VMEM)
    dma = pltpu.SemaphoreType.DMA
    return pl.pallas_call(
        kernel,
        out_shape=jax.ShapeDtypeStruct((ROWS, DH), BF16),
        in_specs=[hbm, hbm, hbm, hbm, smem, hbm, hbm, smem, smem],
        out_specs=vmem,
        scratch_shapes=[
            pltpu.VMEM((ND, ROWS, DH), BF16),
            pltpu.VMEM((ND, ROWS, DH), BF16),
            pltpu.VMEM((ND * DH, DH), BF16),
            pltpu.VMEM((ND * DH, DH), BF16),
            pltpu.VMEM((ND, DH), F32),
            pltpu.VMEM((IMAGES, VT, DH), BF16),
            pltpu.VMEM((IMAGES, VT, DH), BF16),
            pltpu.VMEM((ROWS, DH), F32),
            pltpu.VMEM((ROWS, DH), F32),
            dma((6,)),
            dma((1,)),
            dma((ND + 1,)),
            dma((1,)),
            dma((ND + 1,)),
            dma((2,)),
            dma((2, 9)),
        ],
        compiler_params=pltpu.CompilerParams(
            collective_id=0, has_side_effects=True, vmem_limit_bytes=56 * 1024 * 1024
        ),
        name="gated_cross_attention",
    )(tokens, norm_gain.reshape(ND, DH), query_weight, out_weight, gate_scalar,
      image_keys, image_values, active_image.T, image_slot)


def solution(mesh):
    placed = (
        P("mp", "dp"),
        P(),
        P(None, "dp"),
        P(None, "dp"),
        P(),
        P("mp", None, "dp"),
        P("mp", None, "dp"),
        P(),
        P(),
    )
    return jax.shard_map(body, mesh=mesh, in_specs=placed, out_specs=P("mp", "dp"), check_vma=False)
```

```python
import jax
import jax.numpy as jnp
from jax import lax
from jax.experimental import pallas as pl
from jax.experimental.pallas import tpu as pltpu
from jax.sharding import PartitionSpec as P

MESH = pl.DeviceIdType.MESH
NY, NZ, NX = 4, 16, 4
ND = NY * NZ
ROWS = 64
DH = 128
VT = 64
OWN = 16
HALF = OWN // 2
IMAGES = 128
EPS = 1e-05
F32 = jnp.float32
BF16 = jnp.bfloat16

SPREAD = (
    ((0, 0), ((0, 5), (3, 0), (2, 0), (0, 12), (0, 1), (0, 15))),
    ((3, 0), ((3, 2), (3, 14), (1, 0))),
    ((0, 1), ((0, 4), (3, 1), (1, 1), (2, 1))),
    ((0, 15), ((2, 15), (1, 15), (3, 15))),
    ((2, 0), ((2, 14),)),
    ((0, 12), ((1, 12), (0, 9), (3, 12), (2, 12), (0, 10), (0, 13))),
    ((0, 5), ((0, 6), (2, 5), (1, 5), (3, 5), (0, 8))),
    ((3, 1), ()),
    ((1, 1), ()),
    ((3, 2), ((1, 2), (3, 3), (0, 2), (2, 2))),
    ((3, 14), ((3, 13),)),
    ((3, 15), ()),
    ((1, 15), ()),
    ((2, 14), ((2, 13), (1, 14))),
    ((1, 0), ()),
    ((2, 1), ()),
    ((0, 4), ((2, 4), (0, 3), (1, 4), (3, 4))),
    ((2, 15), ()),
    ((1, 12), ((1, 13), (1, 11))),
    ((3, 12), ((3, 11), (3, 10))),
    ((0, 13), ((0, 14),)),
    ((0, 6), ((2, 6), (3, 6), (1, 6))),
    ((1, 5), ((1, 7),)),
    ((3, 5), ((3, 7),)),
    ((2, 12), ((2, 11),)),
    ((0, 10), ((2, 10), (1, 10), (0, 11))),
    ((2, 5), ((2, 3), (2, 7))),
    ((0, 9), ((3, 9), (2, 9), (1, 9))),
    ((0, 2), ()),
    ((2, 2), ()),
    ((3, 3), ()),
    ((3, 13), ()),
    ((0, 8), ((2, 8), (1, 8), (0, 7), (3, 8))),
    ((1, 2), ()),
    ((2, 13), ()),
    ((1, 14), ()),
    ((0, 3), ()),
    ((1, 4), ((1, 3),)),
    ((1, 13), ()),
    ((3, 4), ()),
    ((1, 11), ()),
    ((2, 4), ()),
    ((0, 14), ()),
    ((3, 11), ()),
    ((1, 6), ()),
    ((3, 6), ()),
    ((2, 11), ()),
    ((2, 6), ()),
    ((0, 11), ()),
    ((1, 10), ()),
    ((3, 9), ()),
    ((3, 10), ()),
    ((1, 9), ()),
    ((2, 10), ()),
    ((1, 7), ()),
    ((2, 3), ()),
    ((3, 8), ()),
    ((3, 7), ()),
    ((0, 7), ()),
    ((1, 8), ()),
    ((2, 9), ()),
    ((2, 7), ()),
    ((2, 8), ()),
    ((1, 3), ()),
)


def kernel(
    tok_h, gain_h, wq_h, wo_h, gate_s, key_h, val_h, act_s, slot_s,
    out_ref,
    tbuf, abuf, wq, wo, gain, kbuf, vbuf, qf, of, pbuf,
    local_sem, t_send, t_recv, a_send, a_recv, kv_send, kv_recv,
):
    dp = lax.axis_index("dp")
    mp = lax.axis_index("mp")
    y, z = dp // NZ, lax.rem(dp, NZ)
    x, core = mp // 2, lax.rem(mp, 2)
    ys = [lax.rem(y + d, NY) * NZ for d in range(NY)]
    zs = [lax.rem(z + d, NZ) for d in range(NZ)]
    xs = [lax.rem(x + d, NX) * 2 for d in range(NX)]

    def block(dy, dz):
        return ys[dy % NY] + zs[dz % NZ]

    def plane_peer(dy, dz):
        return (block(dy, dz), mp)

    def line_peer(px):
        return (dp, xs[px % NX] + core)

    sibling = (dp, xs[0] + (1 - core))

    local = [
        pltpu.make_async_copy(src, dst, local_sem.at[i])
        for i, (src, dst) in enumerate((
            (tok_h, tbuf.at[dp]),
            (gain_h, gain),
            (wq_h, wq),
            (wo_h, wo),
            (key_h, kbuf.at[pl.ds(mp * OWN, OWN)]),
            (val_h, vbuf.at[pl.ds(mp * OWN, OWN)]),
        ))
    ]
    for copy in local:
        copy.start()

    barrier = pltpu.get_barrier_semaphore()
    steps = {((c[0] - p[0]) % NY, (c[1] - p[1]) % NZ) for p, onward in SPREAD for c in onward}
    steps |= {((-a) % NY, (-b) % NZ) for a, b in steps}
    partners = [plane_peer(*step) for step in sorted(steps)]
    partners += [line_peer(1), line_peer(-1), sibling]
    for peer in partners:
        pl.semaphore_signal(barrier, inc=1, device_id=peer, device_id_type=MESH)
    pl.semaphore_wait(barrier, len(partners))

    kv = ((kbuf, key_h), (vbuf, val_h))

    def images(px, same, part=None):
        first = (xs[px % NX] + (core if same else 1 - core)) * OWN
        if part is None:
            return pl.ds(pl.multiple_of(first, OWN), OWN)
        return pl.ds(pl.multiple_of(first + part * HALF, HALF), HALF)

    def kv_copy(which, source, where, peer, sem):
        return pltpu.make_async_remote_copy(
            src_ref=source, dst_ref=kv[which][0].at[where], send_sem=kv_send.at[which],
            recv_sem=kv_recv.at[which, sem], device_id=peer, device_id_type=MESH)

    ARRIVED = ((-1, 0), (-1, 1), (1, 0), (1, 1), (2, 0), (2, 1))

    def kv_own_half(which, px, part):
        source = kv[which][1].at[pl.ds(part * HALF, HALF)]
        kv_copy(which, source, images(0, True, part), line_peer(px), (0 if px == 1 else 2) + part).start()

    def kv_own_sibling(which):
        kv_copy(which, kv[which][1], images(0, True), sibling, 6).start()

    def kv_wait(which, where, sem):
        kv_copy(which, kv[which][0].at[where], where, sibling, sem).wait_recv()

    def kv_arrive(which, sem, onward=None):
        px, part = ARRIVED[sem]
        where = images(px, True, part)
        kv_wait(which, where, sem)
        source = kv[which][0].at[where]
        if onward is not None:
            kv_copy(which, source, where, line_peer(onward), 4 + part).start()
        kv_copy(which, source, where, sibling, 7 + sem).start()

    def kv_finish(which):
        kv_wait(which, images(0, False), 6)
        for sem, (px, part) in enumerate(ARRIVED):
            kv_wait(which, images(px, False, part), 7 + sem)

    index_of = {place: i for i, (place, _) in enumerate(SPREAD)}

    def arrived_block(place):
        return block(-place[0], -place[1])

    def spread(buf, send_sem, recv_sem, i):
        place, onward = SPREAD[i]
        here = buf.at[arrived_block(place)]
        if i > 0:
            pltpu.make_async_remote_copy(
                src_ref=here, dst_ref=here, send_sem=send_sem, recv_sem=recv_sem.at[i],
                device_id=sibling, device_id_type=MESH).wait_recv()
        for target in onward:
            pltpu.make_async_remote_copy(
                src_ref=here, dst_ref=here, send_sem=send_sem, recv_sem=recv_sem.at[index_of[target]],
                device_id=plane_peer(target[0] - place[0], target[1] - place[1]),
                device_id_type=MESH).start()

    def all_sent(buf, send_sem):
        whole = buf.at[pl.ds(0, ND - 1)]
        pltpu.make_async_copy(whole, whole, send_sem).wait()

    local[0].wait()
    spread(tbuf, t_send.at[0], t_recv, 0)
    for which, parts in ((0, (0, 1)), (1, (0,))):
        for part in parts:
            kv_own_half(which, 1, part)
            kv_own_half(which, -1, 1 - part)
        kv_own_sibling(which)

    own = tbuf[dp].astype(F32)
    shift = jnp.broadcast_to(jnp.sum(own, axis=1, keepdims=True) * (1.0 / DH), (ROWS, DH))
    total = own - shift
    square = total * total
    kv_steps = {
        7: ((0, 0, 1), (0, 3, -1)),
        24: ((0, 1, None), (0, 2, None)),
        46: ((1, 0, 1), (1, 3, -1)),
        63: ((0, 4, None), (0, 5, None)),
    }
    for i in range(1, ND):
        spread(tbuf, t_send.at[0], t_recv, i)
        part = tbuf[arrived_block(SPREAD[i][0])].astype(F32) - shift
        total = total + part
        square = square + part * part
        for which, sem, onward in kv_steps.get(i, ()):
            kv_arrive(which, sem, onward)
        if i == 7:
            kv_own_half(1, 1, 1)
            kv_own_half(1, -1, 0)

    drift = jnp.sum(total, axis=1, keepdims=True) * (1.0 / (ND * DH))
    variance = jnp.sum(square, axis=1, keepdims=True) * (1.0 / (ND * DH)) - drift * drift
    mean_b = shift + drift
    scale_b = jnp.broadcast_to(lax.rsqrt(jnp.maximum(variance, 0.0) + EPS), (ROWS, DH))
    local[1].wait()
    local[2].wait()

    def project(i, acc):
        parts = []
        for j in range(4):
            d = i * 4 + j
            g = gain[pl.ds(d, 1), :]
            parts.append((((tbuf[d].astype(F32) - mean_b) * scale_b) * g).astype(BF16))
        lhs = jnp.concatenate(parts, axis=1)
        rhs = wq[pl.ds(pl.multiple_of(i * 4 * DH, 4 * DH), 4 * DH), :]
        return acc + jnp.dot(lhs, rhs, preferred_element_type=F32)

    queries = lax.fori_loop(0, ND // 4, project, jnp.zeros((ROWS, DH), F32), unroll=4)
    qf[...] = queries.astype(BF16).astype(F32)

    kv_arrive(1, 1)
    kv_arrive(1, 2)
    local[4].wait()
    kv_finish(0)

    def slot_of(i, j):
        image = act_s[j % 4, mp * (ROWS // 4) + i * 2 + j // 4]
        return slot_s[image]

    def weigh(i, carry):
        for j in range(8):
            q = qf[pl.ds(i * 8 + j, 1), :]
            s = jnp.sum(kbuf[slot_of(i, j)].astype(F32) * q, axis=1, keepdims=True) * (DH ** -0.5)
            e = jnp.exp(s - jnp.max(s, axis=0, keepdims=True))
            p = (e / jnp.sum(e, axis=0, keepdims=True)).astype(BF16).astype(F32)
            pbuf[i * 8 + j] = jnp.broadcast_to(p, (VT, DH))
        return carry

    lax.fori_loop(0, ROWS // 8, weigh, 0)

    kv_arrive(1, 4)
    kv_arrive(1, 5)
    local[5].wait()
    kv_finish(1)

    def collect(i, carry):
        outs = [
            jnp.sum(pbuf[i * 8 + j] * vbuf[slot_of(i, j)].astype(F32), axis=0, keepdims=True)
            for j in range(8)
        ]
        of[pl.ds(pl.multiple_of(i * 8, 8), 8), :] = jnp.concatenate(outs, axis=0)
        return carry

    lax.fori_loop(0, ROWS // 8, collect, 0)
    abuf[dp] = of[...].astype(BF16)

    final = max(i for i, (_, onward) in enumerate(SPREAD) if onward) + 1
    for i in range(final):
        spread(abuf, a_send.at[0], a_recv, i)
    local[3].wait()

    def project_out(acc, first, last):
        places = [arrived_block(SPREAD[i][0]) for i in range(first, last)]
        lhs = jnp.concatenate([abuf[b] for b in places], axis=1)
        rhs = jnp.concatenate([wo[pl.ds(pl.multiple_of(b * DH, DH), DH), :] for b in places], axis=0)
        return acc + jnp.dot(lhs, rhs, preferred_element_type=F32)

    projected = jnp.zeros((ROWS, DH), F32)
    for first in range(0, final, 8):
        projected = project_out(projected, first, min(first + 8, final))
    for first in range(final, ND, 4):
        last = min(first + 4, ND)
        for i in range(first, last):
            spread(abuf, a_send.at[0], a_recv, i)
        projected = project_out(projected, first, last)
    gate = jnp.tanh(jnp.full((ROWS, DH), gate_s[0], F32))
    out_ref[...] = (tbuf[dp].astype(F32) + gate * projected).astype(BF16)

    all_sent(tbuf, t_send.at[0])
    all_sent(abuf, a_send.at[0])
    for which in (0, 1):
        whole = kv[which][0].at[pl.ds(0, 7 * OWN)]
        pltpu.make_async_copy(whole, whole, kv_send.at[which]).wait()


def body(tokens, norm_gain, query_weight, out_weight, gate_scalar, image_keys, image_values, active_image, image_slot):
    hbm = pl.BlockSpec(memory_space=pltpu.HBM)
    smem = pl.BlockSpec(memory_space=pltpu.SMEM)
    vmem = pl.BlockSpec(memory_space=pltpu.VMEM)
    dma = pltpu.SemaphoreType.DMA
    return pl.pallas_call(
        kernel,
        out_shape=jax.ShapeDtypeStruct((ROWS, DH), BF16),
        in_specs=[hbm, hbm, hbm, hbm, smem, hbm, hbm, smem, smem],
        out_specs=vmem,
        scratch_shapes=[
            pltpu.VMEM((ND, ROWS, DH), BF16),
            pltpu.VMEM((ND, ROWS, DH), BF16),
            pltpu.VMEM((ND * DH, DH), BF16),
            pltpu.VMEM((ND * DH, DH), BF16),
            pltpu.VMEM((ND, DH), F32),
            pltpu.VMEM((IMAGES, VT, DH), BF16),
            pltpu.VMEM((IMAGES, VT, DH), BF16),
            pltpu.VMEM((ROWS, DH), F32),
            pltpu.VMEM((ROWS, DH), F32),
            pltpu.VMEM((ROWS, VT, DH), F32),
            dma((6,)),
            dma((1,)),
            dma((ND,)),
            dma((1,)),
            dma((ND,)),
            dma((2,)),
            dma((2, 13)),
        ],
        compiler_params=pltpu.CompilerParams(
            collective_id=0, has_side_effects=True, vmem_limit_bytes=56 * 1024 * 1024
        ),
        name="gated_cross_attention",
    )(tokens, norm_gain.reshape(ND, DH), query_weight, out_weight, gate_scalar,
      image_keys, image_values, active_image.T, image_slot)


def solution(mesh):
    placed = (
        P("mp", "dp"),
        P(),
        P(None, "dp"),
        P(None, "dp"),
        P(),
        P("mp", None, "dp"),
        P("mp", None, "dp"),
        P(),
        P(),
    )
    return jax.shard_map(body, mesh=mesh, in_specs=placed, out_specs=P("mp", "dp"), check_vma=False)
```

```python
import jax
import jax.numpy as jnp
from jax import lax
from jax.experimental import pallas as pl
from jax.experimental.pallas import tpu as pltpu
from jax.sharding import PartitionSpec as P

MESH = pl.DeviceIdType.MESH
NY, NZ, NX = 4, 16, 4
ND = NY * NZ
ROWS = 64
DH = 128
VT = 64
OWN = 16
HALF = OWN // 2
IMAGES = 128
EPS = 1e-05
F32 = jnp.float32
BF16 = jnp.bfloat16

SPREAD = (
    ((0, 0), ((0, 5), (0, 11), (1, 0), (0, 15), (3, 0), (2, 0), (0, 3))),
    ((1, 0), ((1, 1),)),
    ((3, 0), ((3, 13), (3, 1))),
    ((0, 15), ((0, 1), (2, 15), (1, 15), (0, 13), (0, 14), (3, 15))),
    ((2, 0), ((2, 2),)),
    ((0, 3), ((2, 3), (0, 4), (3, 3), (0, 2), (1, 3))),
    ((0, 11), ((1, 11), (0, 8), (3, 11), (0, 10), (2, 11))),
    ((0, 5), ((0, 7), (1, 5), (3, 5), (2, 5), (0, 6))),
    ((1, 1), ()),
    ((3, 1), ((2, 1),)),
    ((1, 15), ()),
    ((3, 15), ()),
    ((0, 14), ((1, 14), (3, 14))),
    ((2, 15), ((2, 14),)),
    ((0, 13), ((0, 12), (1, 13))),
    ((0, 1), ()),
    ((3, 13), ((2, 13),)),
    ((3, 3), ()),
    ((1, 3), ((1, 4), (1, 2))),
    ((0, 4), ((3, 4), (2, 4))),
    ((0, 2), ()),
    ((2, 2), ((3, 2),)),
    ((2, 3), ()),
    ((1, 11), ((1, 9), (1, 12))),
    ((3, 11), ((3, 9), (3, 12))),
    ((0, 10), ((1, 10), (3, 10))),
    ((1, 5), ((1, 6),)),
    ((0, 6), ((3, 6),)),
    ((3, 5), ()),
    ((0, 7), ((1, 7), (2, 7), (3, 7))),
    ((2, 11), ((2, 9), (2, 10), (2, 12))),
    ((2, 1), ()),
    ((1, 14), ()),
    ((0, 8), ((2, 8), (1, 8), (0, 9), (3, 8))),
    ((2, 5), ((2, 6),)),
    ((3, 14), ()),
    ((2, 14), ()),
    ((1, 13), ()),
    ((0, 12), ()),
    ((2, 13), ()),
    ((1, 4), ()),
    ((1, 2), ()),
    ((3, 4), ()),
    ((3, 2), ()),
    ((1, 12), ()),
    ((2, 4), ()),
    ((3, 12), ()),
    ((1, 10), ()),
    ((3, 10), ()),
    ((1, 9), ()),
    ((1, 6), ()),
    ((3, 6), ()),
    ((1, 7), ()),
    ((3, 9), ()),
    ((2, 12), ()),
    ((3, 7), ()),
    ((0, 9), ()),
    ((1, 8), ()),
    ((2, 10), ()),
    ((2, 6), ()),
    ((3, 8), ()),
    ((2, 7), ()),
    ((2, 8), ()),
    ((2, 9), ()),
)


def kernel(
    tok_h, gain_h, wq_h, wo_h, gate_h, key_h, val_h, act_h, slot_h,
    out_ref,
    tbuf, abuf, wq, wo, gain, kbuf, vbuf, qf, of, pbuf, gate_s, act_s, slot_s,
    local_sem, t_send, t_recv, a_send, a_recv, kv_send, kv_recv,
):
    dp = lax.axis_index("dp")
    mp = lax.axis_index("mp")
    y, z = dp // NZ, lax.rem(dp, NZ)
    x, core = mp // 2, lax.rem(mp, 2)
    ys = [lax.rem(y + d, NY) * NZ for d in range(NY)]
    zs = [lax.rem(z + d, NZ) for d in range(NZ)]
    xs = [lax.rem(x + d, NX) * 2 for d in range(NX)]

    def block(dy, dz):
        return ys[dy % NY] + zs[dz % NZ]

    def plane_peer(dy, dz):
        return (block(dy, dz), mp)

    def line_peer(px):
        return (dp, xs[px % NX] + core)

    sibling = (dp, xs[0] + (1 - core))

    local = [
        pltpu.make_async_copy(src, dst, local_sem.at[i])
        for i, (src, dst) in enumerate((
            (tok_h, tbuf.at[dp]),
            (gain_h, gain),
            (wq_h, wq),
            (wo_h, wo),
            (key_h, kbuf.at[pl.ds(mp * OWN, OWN)]),
            (val_h, vbuf.at[pl.ds(mp * OWN, OWN)]),
            (gate_h, gate_s),
            (act_h, act_s),
            (slot_h, slot_s),
        ))
    ]
    for copy in local:
        copy.start()

    barrier = pltpu.get_barrier_semaphore()
    steps = {((c[0] - p[0]) % NY, (c[1] - p[1]) % NZ) for p, onward in SPREAD for c in onward}
    steps |= {((-a) % NY, (-b) % NZ) for a, b in steps}
    partners = [plane_peer(*step) for step in sorted(steps)]
    partners += [line_peer(1), line_peer(-1), sibling]
    for peer in partners:
        pl.semaphore_signal(barrier, inc=1, device_id=peer, device_id_type=MESH)
    pl.semaphore_wait(barrier, len(partners))

    kv = ((kbuf, key_h), (vbuf, val_h))

    def images(px, same, part=None):
        first = (xs[px % NX] + (core if same else 1 - core)) * OWN
        if part is None:
            return pl.ds(pl.multiple_of(first, OWN), OWN)
        return pl.ds(pl.multiple_of(first + part * HALF, HALF), HALF)

    def kv_copy(which, source, where, peer, sem):
        return pltpu.make_async_remote_copy(
            src_ref=source, dst_ref=kv[which][0].at[where], send_sem=kv_send.at[which],
            recv_sem=kv_recv.at[which, sem], device_id=peer, device_id_type=MESH)

    ARRIVED = ((-1, 0), (-1, 1), (1, 0), (1, 1), (2, 0), (2, 1))

    def kv_own_half(which, px, part):
        source = kv[which][1].at[pl.ds(part * HALF, HALF)]
        kv_copy(which, source, images(0, True, part), line_peer(px), (0 if px == 1 else 2) + part).start()

    def kv_own_sibling(which):
        kv_copy(which, kv[which][1], images(0, True), sibling, 6).start()

    def kv_wait(which, where, sem):
        kv_copy(which, kv[which][0].at[where], where, sibling, sem).wait_recv()

    def kv_arrive(which, sem, onward=None):
        px, part = ARRIVED[sem]
        where = images(px, True, part)
        kv_wait(which, where, sem)
        source = kv[which][0].at[where]
        if onward is not None:
            kv_copy(which, source, where, line_peer(onward), 4 + part).start()
        kv_copy(which, source, where, sibling, 7 + sem).start()

    def kv_finish(which):
        kv_wait(which, images(0, False), 6)
        for sem, (px, part) in enumerate(ARRIVED):
            kv_wait(which, images(px, False, part), 7 + sem)

    index_of = {place: i for i, (place, _) in enumerate(SPREAD)}

    def arrived_block(place):
        return block(-place[0], -place[1])

    def spread(buf, send_sem, recv_sem, i):
        place, onward = SPREAD[i]
        here = buf.at[arrived_block(place)]
        if i > 0:
            pltpu.make_async_remote_copy(
                src_ref=here, dst_ref=here, send_sem=send_sem, recv_sem=recv_sem.at[i],
                device_id=sibling, device_id_type=MESH).wait_recv()
        for target in onward:
            pltpu.make_async_remote_copy(
                src_ref=here, dst_ref=here, send_sem=send_sem, recv_sem=recv_sem.at[index_of[target]],
                device_id=plane_peer(target[0] - place[0], target[1] - place[1]),
                device_id_type=MESH).start()

    def all_sent(buf, send_sem):
        whole = buf.at[pl.ds(0, ND - 1)]
        pltpu.make_async_copy(whole, whole, send_sem).wait()

    local[0].wait()
    spread(tbuf, t_send.at[0], t_recv, 0)
    for which, parts in ((0, (0, 1)), (1, (0,))):
        for part in parts:
            kv_own_half(which, 1, part)
            kv_own_half(which, -1, 1 - part)
        kv_own_sibling(which)

    own = tbuf[dp].astype(F32)
    shift = jnp.broadcast_to(jnp.sum(own, axis=1, keepdims=True) * (1.0 / DH), (ROWS, DH))
    total = own - shift
    square = total * total
    kv_steps = {
        8: ((0, 0, 1), (0, 3, -1)),
        26: ((0, 1, None), (0, 2, None)),
        46: ((1, 0, 1), (1, 3, -1)),
        63: ((0, 4, None), (0, 5, None)),
    }
    for i in range(1, ND):
        spread(tbuf, t_send.at[0], t_recv, i)
        part = tbuf[arrived_block(SPREAD[i][0])].astype(F32) - shift
        total = total + part
        square = square + part * part
        for which, sem, onward in kv_steps.get(i, ()):
            kv_arrive(which, sem, onward)
        if i == 8:
            kv_own_half(1, 1, 1)
            kv_own_half(1, -1, 0)

    drift = jnp.sum(total, axis=1, keepdims=True) * (1.0 / (ND * DH))
    variance = jnp.sum(square, axis=1, keepdims=True) * (1.0 / (ND * DH)) - drift * drift
    mean_b = shift + drift
    scale_b = jnp.broadcast_to(lax.rsqrt(jnp.maximum(variance, 0.0) + EPS), (ROWS, DH))
    local[1].wait()
    local[2].wait()

    def project(i, acc):
        parts = []
        for j in range(4):
            d = i * 4 + j
            g = gain[pl.ds(d, 1), :]
            parts.append((((tbuf[d].astype(F32) - mean_b) * scale_b) * g).astype(BF16))
        lhs = jnp.concatenate(parts, axis=1)
        rhs = wq[pl.ds(pl.multiple_of(i * 4 * DH, 4 * DH), 4 * DH), :]
        return acc + jnp.dot(lhs, rhs, preferred_element_type=F32)

    queries = lax.fori_loop(0, ND // 4, project, jnp.zeros((ROWS, DH), F32), unroll=4)
    qf[...] = queries.astype(BF16).astype(F32)

    kv_arrive(1, 1)
    kv_arrive(1, 2)
    for i in (4, 7, 8):
        local[i].wait()
    kv_finish(0)

    def slot_of(i, j):
        image = act_s[j % 4, mp * (ROWS // 4) + i * 2 + j // 4]
        return slot_s[image]

    def weigh(i, carry):
        for j in range(8):
            q = qf[pl.ds(i * 8 + j, 1), :]
            s = jnp.sum(kbuf[slot_of(i, j)].astype(F32) * q, axis=1, keepdims=True) * (DH ** -0.5)
            e = jnp.exp(s - jnp.max(s, axis=0, keepdims=True))
            p = (e / jnp.sum(e, axis=0, keepdims=True)).astype(BF16).astype(F32)
            pbuf[i * 8 + j] = jnp.broadcast_to(p, (VT, DH))
        return carry

    lax.fori_loop(0, ROWS // 8, weigh, 0)

    kv_arrive(1, 4)
    kv_arrive(1, 5)
    local[5].wait()
    kv_finish(1)

    def collect(i, carry):
        outs = [
            jnp.sum(pbuf[i * 8 + j] * vbuf[slot_of(i, j)].astype(F32), axis=0, keepdims=True)
            for j in range(8)
        ]
        of[pl.ds(pl.multiple_of(i * 8, 8), 8), :] = jnp.concatenate(outs, axis=0)
        return carry

    lax.fori_loop(0, ROWS // 8, collect, 0)
    abuf[dp] = of[...].astype(BF16)

    final = max(i for i, (_, onward) in enumerate(SPREAD) if onward) + 1
    for i in range(final):
        spread(abuf, a_send.at[0], a_recv, i)
    local[3].wait()

    def project_out(acc, first, last):
        places = [arrived_block(SPREAD[i][0]) for i in range(first, last)]
        lhs = jnp.concatenate([abuf[b] for b in places], axis=1)
        rhs = jnp.concatenate([wo[pl.ds(pl.multiple_of(b * DH, DH), DH), :] for b in places], axis=0)
        return acc + jnp.dot(lhs, rhs, preferred_element_type=F32)

    projected = jnp.zeros((ROWS, DH), F32)
    for first in range(0, final, 8):
        projected = project_out(projected, first, min(first + 8, final))
    for first in range(final, ND, 4):
        last = min(first + 4, ND)
        for i in range(first, last):
            spread(abuf, a_send.at[0], a_recv, i)
        projected = project_out(projected, first, last)
    local[6].wait()
    gate = jnp.tanh(jnp.full((ROWS, DH), gate_s[0], F32))
    out_ref[...] = (tbuf[dp].astype(F32) + gate * projected).astype(BF16)

    all_sent(tbuf, t_send.at[0])
    all_sent(abuf, a_send.at[0])
    for which in (0, 1):
        whole = kv[which][0].at[pl.ds(0, 7 * OWN)]
        pltpu.make_async_copy(whole, whole, kv_send.at[which]).wait()


def body(tokens, norm_gain, query_weight, out_weight, gate_scalar, image_keys, image_values, active_image, image_slot):
    hbm = pl.BlockSpec(memory_space=pltpu.HBM)
    vmem = pl.BlockSpec(memory_space=pltpu.VMEM)
    dma = pltpu.SemaphoreType.DMA
    return pl.pallas_call(
        kernel,
        out_shape=pltpu.VMEM((ROWS, DH), BF16),
        in_specs=[hbm] * 9,
        out_specs=vmem,
        scratch_shapes=[
            pltpu.VMEM((ND, ROWS, DH), BF16),
            pltpu.VMEM((ND, ROWS, DH), BF16),
            pltpu.VMEM((ND * DH, DH), BF16),
            pltpu.VMEM((ND * DH, DH), BF16),
            pltpu.VMEM((ND, DH), F32),
            pltpu.VMEM((IMAGES, VT, DH), BF16),
            pltpu.VMEM((IMAGES, VT, DH), BF16),
            pltpu.VMEM((ROWS, DH), F32),
            pltpu.VMEM((ROWS, DH), F32),
            pltpu.VMEM((ROWS, VT, DH), F32),
            pltpu.SMEM((1,), F32),
            pltpu.SMEM((4, 128), jnp.int32),
            pltpu.SMEM((IMAGES,), jnp.int32),
            dma((9,)),
            dma((1,)),
            dma((ND,)),
            dma((1,)),
            dma((ND,)),
            dma((2,)),
            dma((2, 13)),
        ],
        compiler_params=pltpu.CompilerParams(
            collective_id=0, has_side_effects=True, vmem_limit_bytes=56 * 1024 * 1024
        ),
        name="gated_cross_attention",
    )(tokens, norm_gain.reshape(ND, DH), query_weight, out_weight, gate_scalar,
      image_keys, image_values, active_image.T, image_slot)


def solution(mesh):
    placed = (
        P("mp", "dp"),
        P(),
        P(None, "dp"),
        P(None, "dp"),
        P(),
        P("mp", None, "dp"),
        P("mp", None, "dp"),
        P(),
        P(),
    )
    return jax.shard_map(body, mesh=mesh, in_specs=placed, out_specs=P("mp", "dp"), check_vma=False)
```

```python
import jax
import jax.numpy as jnp
from jax import lax
from jax.experimental import pallas as pl
from jax.experimental.pallas import tpu as pltpu
from jax.sharding import PartitionSpec as P

MESH = pl.DeviceIdType.MESH
NY, NZ, NX = 4, 16, 4
ND = NY * NZ
ROWS = 64
DH = 128
VT = 64
OWN = 16
HALF = OWN // 2
IMAGES = 128
EPS = 1e-05
F32 = jnp.float32
BF16 = jnp.bfloat16

NEAR_SPREAD = (
    ((0, 0), ((0, 3), (0, 15), (1, 0), (0, 13), (3, 0), (0, 14))),
    ((0, 15), ((3, 15), (0, 12), (2, 15), (0, 1))),
    ((1, 0), ((1, 1),)),
    ((3, 0), ((2, 0),)),
    ((0, 3), ((0, 6), (1, 3), (2, 3))),
    ((0, 14), ((1, 14), (3, 14), (2, 14))),
    ((0, 13), ((3, 13), (0, 11), (2, 13), (1, 13), (0, 10))),
    ((2, 0), ((2, 1),)),
    ((2, 15), ((1, 15),)),
    ((0, 1), ((0, 2), (3, 1))),
    ((1, 3), ((1, 2), (1, 5), (1, 4), (3, 3))),
    ((0, 12), ((2, 12), (1, 12), (3, 12))),
    ((3, 13), ((3, 11),)),
    ((0, 6), ((0, 8), (1, 6), (2, 6), (3, 6), (0, 5), (0, 7))),
    ((0, 11), ((1, 11), (2, 11))),
    ((2, 13), ((2, 10),)),
    ((2, 1), ((2, 2),)),
    ((0, 10), ((3, 10), (1, 10), (0, 9))),
    ((0, 2), ((3, 2),)),
    ((1, 4), ((2, 4), (0, 4))),
    ((1, 5), ((2, 5), (3, 5))),
    ((3, 3), ((3, 4),)),
    ((2, 12), ((2, 9),)),
    ((1, 6), ((1, 8), (1, 7))),
    ((0, 7), ((3, 7),)),
    ((0, 8), ((2, 8), (3, 8))),
    ((2, 6), ((2, 7),)),
    ((3, 10), ((3, 9),)),
    ((0, 9), ((1, 9),)),
    ((3, 15), ()),
    ((1, 1), ()),
    ((1, 14), ()),
    ((3, 14), ()),
    ((2, 3), ()),
    ((1, 13), ()),
    ((2, 14), ()),
    ((1, 15), ()),
    ((3, 1), ()),
    ((1, 2), ()),
    ((1, 12), ()),
    ((3, 12), ()),
    ((0, 5), ()),
    ((1, 11), ()),
    ((3, 6), ()),
    ((3, 11), ()),
    ((2, 2), ()),
    ((1, 10), ()),
    ((2, 11), ()),
    ((3, 2), ()),
    ((2, 4), ()),
    ((2, 10), ()),
    ((0, 4), ()),
    ((2, 5), ()),
    ((3, 4), ()),
    ((3, 5), ()),
    ((3, 7), ()),
    ((1, 7), ()),
    ((1, 8), ()),
    ((3, 8), ()),
    ((2, 9), ()),
    ((2, 7), ()),
    ((1, 9), ()),
    ((3, 9), ()),
    ((2, 8), ()),
)
FAR_SPREAD = (
    ((0, 0), ((0, 5), (0, 11), (1, 0), (0, 15), (3, 0), (2, 0), (0, 3))),
    ((1, 0), ((1, 1),)),
    ((3, 0), ((3, 13), (3, 1))),
    ((0, 15), ((0, 1), (2, 15), (1, 15), (0, 13), (0, 14), (3, 15))),
    ((2, 0), ((2, 2),)),
    ((0, 3), ((2, 3), (0, 4), (3, 3), (0, 2), (1, 3))),
    ((0, 11), ((1, 11), (0, 8), (3, 11), (0, 10), (2, 11))),
    ((0, 5), ((0, 7), (1, 5), (3, 5), (2, 5), (0, 6))),
    ((3, 1), ((2, 1),)),
    ((0, 14), ((1, 14), (3, 14))),
    ((2, 15), ((2, 14),)),
    ((0, 13), ((0, 12), (1, 13))),
    ((3, 13), ((2, 13),)),
    ((1, 3), ((1, 4), (1, 2))),
    ((0, 4), ((3, 4), (2, 4))),
    ((2, 2), ((3, 2),)),
    ((1, 11), ((1, 9), (1, 12))),
    ((3, 11), ((3, 9), (3, 12))),
    ((0, 10), ((1, 10), (3, 10))),
    ((0, 6), ((3, 6),)),
    ((1, 5), ((1, 6),)),
    ((0, 7), ((1, 7), (2, 7), (3, 7))),
    ((2, 11), ((2, 9), (2, 10), (2, 12))),
    ((0, 8), ((2, 8), (1, 8), (0, 9), (3, 8))),
    ((2, 5), ((2, 6),)),
    ((1, 1), ()),
    ((1, 15), ()),
    ((3, 15), ()),
    ((0, 1), ()),
    ((3, 3), ()),
    ((0, 2), ()),
    ((2, 3), ()),
    ((3, 5), ()),
    ((2, 1), ()),
    ((1, 14), ()),
    ((3, 14), ()),
    ((2, 14), ()),
    ((1, 13), ()),
    ((0, 12), ()),
    ((2, 13), ()),
    ((1, 4), ()),
    ((1, 2), ()),
    ((3, 4), ()),
    ((3, 2), ()),
    ((1, 12), ()),
    ((2, 4), ()),
    ((3, 12), ()),
    ((1, 10), ()),
    ((3, 10), ()),
    ((1, 9), ()),
    ((1, 6), ()),
    ((3, 6), ()),
    ((1, 7), ()),
    ((3, 9), ()),
    ((2, 12), ()),
    ((3, 7), ()),
    ((0, 9), ()),
    ((1, 8), ()),
    ((2, 10), ()),
    ((2, 6), ()),
    ((3, 8), ()),
    ((2, 7), ()),
    ((2, 8), ()),
    ((2, 9), ()),
)


def kernel(
    tok_h, gain_h, wq_h, wo_h, gate_h, key_h, val_h, act_h, slot_h,
    out_ref,
    tbuf, abuf, wq, wo, gain, kbuf, vbuf, qf, of, pbuf, gate_s, act_s, slot_s,
    local_sem, t_send, t_recv, a_send, a_recv, kv_send, kv_recv,
):
    dp = lax.axis_index("dp")
    mp = lax.axis_index("mp")
    y, z = dp // NZ, lax.rem(dp, NZ)
    x, core = mp // 2, lax.rem(mp, 2)
    ys = [lax.rem(y + d, NY) * NZ for d in range(NY)]
    zs = [lax.rem(z + d, NZ) for d in range(NZ)]
    xs = [lax.rem(x + d, NX) * 2 for d in range(NX)]

    def block(dy, dz):
        return ys[dy % NY] + zs[dz % NZ]

    def plane_peer(dy, dz):
        return (block(dy, dz), mp)

    def line_peer(px):
        return (dp, xs[px % NX] + core)

    sibling = (dp, xs[0] + (1 - core))

    local = [
        pltpu.make_async_copy(src, dst, local_sem.at[i])
        for i, (src, dst) in enumerate((
            (tok_h, tbuf.at[dp]),
            (gain_h, gain),
            (wq_h, wq),
            (wo_h, wo),
            (key_h, kbuf.at[pl.ds(mp * OWN, OWN)]),
            (val_h, vbuf.at[pl.ds(mp * OWN, OWN)]),
            (gate_h, gate_s),
            (act_h, act_s),
            (slot_h, slot_s),
        ))
    ]
    for copy in local:
        copy.start()

    barrier = pltpu.get_barrier_semaphore()
    steps = {((c[0] - p[0]) % NY, (c[1] - p[1]) % NZ) for p, onward in NEAR_SPREAD for c in onward}
    steps |= {((-a) % NY, (-b) % NZ) for a, b in steps}
    partners = [plane_peer(*step) for step in sorted(steps)]
    partners += [line_peer(1), line_peer(-1), sibling]
    for peer in partners:
        pl.semaphore_signal(barrier, inc=1, device_id=peer, device_id_type=MESH)
    pl.semaphore_wait(barrier, len(partners))

    kv = ((kbuf, key_h), (vbuf, val_h))

    def images(px, same, part=None):
        first = (xs[px % NX] + (core if same else 1 - core)) * OWN
        if part is None:
            return pl.ds(pl.multiple_of(first, OWN), OWN)
        return pl.ds(pl.multiple_of(first + part * HALF, HALF), HALF)

    def kv_copy(which, source, where, peer, sem):
        return pltpu.make_async_remote_copy(
            src_ref=source, dst_ref=kv[which][0].at[where], send_sem=kv_send.at[which],
            recv_sem=kv_recv.at[which, sem], device_id=peer, device_id_type=MESH)

    ARRIVED = ((-1, 0), (-1, 1), (1, 0), (1, 1), (2, 0), (2, 1))

    def kv_own_half(which, px, part):
        source = kv[which][1].at[pl.ds(part * HALF, HALF)]
        kv_copy(which, source, images(0, True, part), line_peer(px), (0 if px == 1 else 2) + part).start()

    def kv_own_sibling(which):
        kv_copy(which, kv[which][1], images(0, True), sibling, 6).start()

    def kv_wait(which, where, sem):
        kv_copy(which, kv[which][0].at[where], where, sibling, sem).wait_recv()

    def kv_arrive(which, sem, onward=None):
        px, part = ARRIVED[sem]
        where = images(px, True, part)
        kv_wait(which, where, sem)
        source = kv[which][0].at[where]
        if onward is not None:
            kv_copy(which, source, where, line_peer(onward), 4 + part).start()
        kv_copy(which, source, where, sibling, 7 + sem).start()

    def kv_finish(which):
        kv_wait(which, images(0, False), 6)
        for sem, (px, part) in enumerate(ARRIVED):
            kv_wait(which, images(px, False, part), 7 + sem)

    def arrived_block(place):
        return block(-place[0], -place[1])

    def spread(tree, buf, send_sem, recv_sem, i):
        place, onward = tree[i]
        index_of = {node: k for k, (node, _) in enumerate(tree)}
        here = buf.at[arrived_block(place)]
        if i > 0:
            pltpu.make_async_remote_copy(
                src_ref=here, dst_ref=here, send_sem=send_sem, recv_sem=recv_sem.at[i],
                device_id=sibling, device_id_type=MESH).wait_recv()
        for target in onward:
            pltpu.make_async_remote_copy(
                src_ref=here, dst_ref=here, send_sem=send_sem, recv_sem=recv_sem.at[index_of[target]],
                device_id=plane_peer(target[0] - place[0], target[1] - place[1]),
                device_id_type=MESH).start()

    def all_sent(buf, send_sem):
        whole = buf.at[pl.ds(0, ND - 1)]
        pltpu.make_async_copy(whole, whole, send_sem).wait()

    local[0].wait()
    spread(NEAR_SPREAD, tbuf, t_send.at[0], t_recv, 0)
    for which, parts in ((0, (0, 1)), (1, (0,))):
        for part in parts:
            kv_own_half(which, 1, part)
            kv_own_half(which, -1, 1 - part)
        kv_own_sibling(which)

    own = tbuf[dp].astype(F32)
    shift = jnp.broadcast_to(jnp.sum(own, axis=1, keepdims=True) * (1.0 / DH), (ROWS, DH))
    total = own - shift
    square = total * total
    kv_steps = {
        7: ((0, 0, 1), (0, 3, -1)),
        15: ((0, 1, None), (0, 2, None)),
        24: ((1, 0, 1), (1, 3, -1)),
        54: ((0, 4, None), (0, 5, None)),
    }
    for i in range(1, ND):
        spread(NEAR_SPREAD, tbuf, t_send.at[0], t_recv, i)
        part = tbuf[arrived_block(NEAR_SPREAD[i][0])].astype(F32) - shift
        total = total + part
        square = square + part * part
        for which, sem, onward in kv_steps.get(i, ()):
            kv_arrive(which, sem, onward)
        if i == 7:
            kv_own_half(1, 1, 1)
            kv_own_half(1, -1, 0)

    drift = jnp.sum(total, axis=1, keepdims=True) * (1.0 / (ND * DH))
    variance = jnp.sum(square, axis=1, keepdims=True) * (1.0 / (ND * DH)) - drift * drift
    mean_b = shift + drift
    scale_b = jnp.broadcast_to(lax.rsqrt(jnp.maximum(variance, 0.0) + EPS), (ROWS, DH))
    local[1].wait()
    local[2].wait()

    def project(i, acc):
        parts = []
        for j in range(4):
            d = i * 4 + j
            g = gain[pl.ds(d, 1), :]
            parts.append((((tbuf[d].astype(F32) - mean_b) * scale_b) * g).astype(BF16))
        lhs = jnp.concatenate(parts, axis=1)
        rhs = wq[pl.ds(pl.multiple_of(i * 4 * DH, 4 * DH), 4 * DH), :]
        return acc + jnp.dot(lhs, rhs, preferred_element_type=F32)

    queries = lax.fori_loop(0, ND // 4, project, jnp.zeros((ROWS, DH), F32), unroll=4)
    qf[...] = queries.astype(BF16).astype(F32)

    kv_arrive(1, 1)
    kv_arrive(1, 2)
    for i in (4, 7, 8):
        local[i].wait()
    kv_finish(0)

    def slot_of(i, j):
        image = act_s[j % 4, mp * (ROWS // 4) + i * 2 + j // 4]
        return slot_s[image]

    def weigh(i, carry):
        for j in range(8):
            q = qf[pl.ds(i * 8 + j, 1), :]
            s = jnp.sum(kbuf[slot_of(i, j)].astype(F32) * q, axis=1, keepdims=True) * (DH ** -0.5)
            e = jnp.exp(s - jnp.max(s, axis=0, keepdims=True))
            p = (e / jnp.sum(e, axis=0, keepdims=True)).astype(BF16).astype(F32)
            pbuf[i * 8 + j] = jnp.broadcast_to(p, (VT, DH))
        return carry

    lax.fori_loop(0, ROWS // 8, weigh, 0)

    kv_arrive(1, 4)
    kv_arrive(1, 5)
    local[5].wait()
    kv_finish(1)

    def collect(i, carry):
        outs = [
            jnp.sum(pbuf[i * 8 + j] * vbuf[slot_of(i, j)].astype(F32), axis=0, keepdims=True)
            for j in range(8)
        ]
        of[pl.ds(pl.multiple_of(i * 8, 8), 8), :] = jnp.concatenate(outs, axis=0)
        return carry

    lax.fori_loop(0, ROWS // 8, collect, 0)
    abuf[dp] = of[...].astype(BF16)

    final = max(i for i, (_, onward) in enumerate(FAR_SPREAD) if onward) + 1
    for i in range(final):
        spread(FAR_SPREAD, abuf, a_send.at[0], a_recv, i)
    local[3].wait()

    def project_out(acc, first, last):
        places = [arrived_block(FAR_SPREAD[i][0]) for i in range(first, last)]
        lhs = jnp.concatenate([abuf[b] for b in places], axis=1)
        rhs = jnp.concatenate([wo[pl.ds(pl.multiple_of(b * DH, DH), DH), :] for b in places], axis=0)
        return acc + jnp.dot(lhs, rhs, preferred_element_type=F32)

    projected = jnp.zeros((ROWS, DH), F32)
    for first in range(0, final, 8):
        projected = project_out(projected, first, min(first + 8, final))
    for first in range(final, ND, 4):
        last = min(first + 4, ND)
        for i in range(first, last):
            spread(FAR_SPREAD, abuf, a_send.at[0], a_recv, i)
        projected = project_out(projected, first, last)
    local[6].wait()
    gate = jnp.tanh(jnp.full((ROWS, DH), gate_s[0], F32))
    out_ref[...] = (tbuf[dp].astype(F32) + gate * projected).astype(BF16)

    all_sent(tbuf, t_send.at[0])
    all_sent(abuf, a_send.at[0])
    for which in (0, 1):
        whole = kv[which][0].at[pl.ds(0, 7 * OWN)]
        pltpu.make_async_copy(whole, whole, kv_send.at[which]).wait()


def body(tokens, norm_gain, query_weight, out_weight, gate_scalar, image_keys, image_values, active_image, image_slot):
    hbm = pl.BlockSpec(memory_space=pltpu.HBM)
    vmem = pl.BlockSpec(memory_space=pltpu.VMEM)
    dma = pltpu.SemaphoreType.DMA
    return pl.pallas_call(
        kernel,
        out_shape=pltpu.VMEM((ROWS, DH), BF16),
        in_specs=[hbm] * 9,
        out_specs=vmem,
        scratch_shapes=[
            pltpu.VMEM((ND, ROWS, DH), BF16),
            pltpu.VMEM((ND, ROWS, DH), BF16),
            pltpu.VMEM((ND * DH, DH), BF16),
            pltpu.VMEM((ND * DH, DH), BF16),
            pltpu.VMEM((ND, DH), F32),
            pltpu.VMEM((IMAGES, VT, DH), BF16),
            pltpu.VMEM((IMAGES, VT, DH), BF16),
            pltpu.VMEM((ROWS, DH), F32),
            pltpu.VMEM((ROWS, DH), F32),
            pltpu.VMEM((ROWS, VT, DH), F32),
            pltpu.SMEM((1,), F32),
            pltpu.SMEM((4, 128), jnp.int32),
            pltpu.SMEM((IMAGES,), jnp.int32),
            dma((9,)),
            dma((1,)),
            dma((ND,)),
            dma((1,)),
            dma((ND,)),
            dma((2,)),
            dma((2, 13)),
        ],
        compiler_params=pltpu.CompilerParams(
            collective_id=0, has_side_effects=True, vmem_limit_bytes=56 * 1024 * 1024
        ),
        name="gated_cross_attention",
    )(tokens, norm_gain.reshape(ND, DH), query_weight, out_weight, gate_scalar,
      image_keys, image_values, active_image.T, image_slot)


def solution(mesh):
    placed = (
        P("mp", "dp"),
        P(),
        P(None, "dp"),
        P(None, "dp"),
        P(),
        P("mp", None, "dp"),
        P("mp", None, "dp"),
        P(),
        P(),
    )
    return jax.shard_map(body, mesh=mesh, in_specs=placed, out_specs=P("mp", "dp"), check_vma=False)
```

```python
import jax
import jax.numpy as jnp
from jax import lax
from jax.experimental import pallas as pl
from jax.experimental.pallas import tpu as pltpu
from jax.sharding import PartitionSpec as P

MESH = pl.DeviceIdType.MESH
NY, NZ, NX = 4, 16, 4
ND = NY * NZ
ROWS = 64
DH = 128
VT = 64
OWN = 16
HALF = OWN // 2
IMAGES = 128
EPS = 1e-05
F32 = jnp.float32
BF16 = jnp.bfloat16

NEAR_SPREAD = (
    ((0, 0), (((0, 0), (0, 14)), ((0, 0), (1, 0)), ((0, 0), (0, 2)), ((0, 0), (3, 0)), ((0, 0), (0, 1)))),
    ((1, 0), (((1, 0), (1, 1)),)),
    ((3, 0), (((3, 0), (2, 0)), ((3, 0), (3, 15)), ((3, 0), (3, 1)))),
    ((0, 14), (((0, 14), (3, 14)), ((0, 14), (1, 14)))),
    ((0, 2), (((0, 14), (0, 10)), ((0, 2), (0, 6)), ((0, 2), (0, 4)), ((0, 2), (2, 2)), ((0, 2), (3, 2)), ((0, 2), (1, 2)))),
    ((1, 1), (((1, 1), (2, 1)),)),
    ((3, 15), (((3, 15), (1, 15)), ((3, 15), (0, 15)), ((3, 15), (2, 15)))),
    ((3, 1), (((3, 1), (3, 3)),)),
    ((3, 14), (((3, 14), (3, 12)), ((3, 14), (3, 13)))),
    ((1, 14), (((1, 14), (2, 14)), ((1, 14), (1, 13)))),
    ((1, 2), (((1, 2), (1, 3)),)),
    ((2, 2), (((2, 2), (2, 3)),)),
    ((0, 4), (((0, 4), (0, 5)), ((0, 4), (3, 4)), ((0, 4), (1, 4)), ((0, 4), (0, 3)))),
    ((0, 10), (((0, 10), (0, 8)), ((0, 10), (3, 10)), ((0, 10), (1, 10)), ((0, 10), (0, 11)), ((0, 10), (2, 10)))),
    ((0, 6), (((0, 6), (0, 7)), ((0, 6), (0, 9)), ((0, 6), (2, 6)), ((0, 6), (3, 6)), ((0, 6), (1, 6)))),
    ((2, 15), (((2, 15), (2, 13)),)),
    ((2, 14), (((2, 14), (2, 11)),)),
    ((1, 13), (((1, 13), (0, 13)), ((1, 13), (1, 12)))),
    ((2, 3), (((2, 3), (2, 5)),)),
    ((3, 12), (((3, 12), (0, 12)), ((3, 12), (2, 12)))),
    ((3, 4), (((3, 4), (2, 4)),)),
    ((0, 5), (((0, 5), (1, 5)), ((0, 5), (3, 5)))),
    ((3, 10), (((3, 10), (3, 11)), ((3, 10), (3, 9)))),
    ((1, 10), (((1, 10), (1, 9)),)),
    ((0, 11), (((0, 11), (1, 11)),)),
    ((0, 7), (((0, 7), (3, 7)),)),
    ((0, 8), (((0, 8), (2, 8)), ((0, 8), (1, 8)), ((0, 8), (3, 8)))),
    ((1, 6), (((1, 6), (1, 7)),)),
    ((2, 10), (((2, 10), (2, 9)),)),
    ((2, 6), (((2, 6), (2, 7)),)),
    ((0, 1), ()),
    ((2, 0), ()),
    ((3, 2), ()),
    ((2, 1), ()),
    ((0, 15), ()),
    ((1, 15), ()),
    ((3, 3), ()),
    ((3, 13), ()),
    ((1, 3), ()),
    ((1, 4), ()),
    ((0, 3), ()),
    ((3, 6), ()),
    ((2, 13), ()),
    ((0, 13), ()),
    ((0, 9), ()),
    ((1, 12), ()),
    ((0, 12), ()),
    ((2, 12), ()),
    ((1, 5), ()),
    ((2, 4), ()),
    ((3, 11), ()),
    ((3, 9), ()),
    ((3, 5), ()),
    ((1, 11), ()),
    ((2, 5), ()),
    ((2, 11), ()),
    ((3, 7), ()),
    ((1, 9), ()),
    ((1, 7), ()),
    ((3, 8), ()),
    ((1, 8), ()),
    ((2, 9), ()),
    ((2, 7), ()),
    ((2, 8), ()),
)
FAR_SPREAD = (
    ((0, 0), (((0, 0), (0, 11)), ((0, 0), (3, 0)), ((0, 0), (2, 0)), ((0, 0), (0, 1)), ((0, 0), (0, 15)), ((0, 0), (0, 5)), ((0, 0), (0, 2)), ((0, 0), (1, 0)))),
    ((3, 0), (((3, 0), (3, 13)),)),
    ((0, 1), (((0, 1), (3, 1)), ((0, 1), (1, 1)))),
    ((0, 15), (((0, 15), (2, 15)), ((0, 15), (0, 14)), ((0, 15), (3, 15)), ((0, 15), (1, 15)))),
    ((1, 0), (((1, 0), (1, 3)), ((1, 0), (1, 14)))),
    ((2, 0), (((2, 0), (2, 1)),)),
    ((0, 2), (((0, 2), (2, 2)), ((0, 2), (0, 4)), ((0, 2), (3, 2)), ((0, 2), (1, 2)))),
    ((0, 11), (((0, 11), (0, 8)), ((0, 11), (2, 11)), ((0, 11), (3, 11)), ((0, 11), (1, 11)), ((0, 11), (0, 9)), ((0, 11), (0, 12)))),
    ((0, 5), (((0, 5), (2, 5)), ((0, 5), (1, 5)), ((0, 5), (0, 6)), ((0, 5), (3, 5)), ((0, 5), (0, 7)))),
    ((0, 14), (((0, 14), (3, 14)),)),
    ((2, 1), (((2, 1), (2, 4)),)),
    ((1, 14), (((1, 14), (2, 14)), ((1, 14), (1, 13)), ((1, 14), (1, 12)))),
    ((3, 13), (((3, 13), (2, 13)), ((3, 13), (3, 12)))),
    ((1, 3), (((1, 3), (3, 3)), ((1, 3), (0, 3)))),
    ((2, 2), (((2, 2), (2, 3)),)),
    ((0, 4), (((0, 4), (1, 4)), ((0, 4), (3, 4)))),
    ((1, 11), (((1, 11), (1, 10)),)),
    ((0, 12), (((0, 12), (0, 13)),)),
    ((3, 11), (((3, 11), (3, 10)),)),
    ((0, 6), (((0, 6), (3, 6)), ((0, 6), (1, 6)))),
    ((2, 11), (((2, 11), (2, 12)), ((2, 11), (2, 10)), ((2, 11), (2, 9)))),
    ((0, 9), (((0, 9), (0, 10)), ((0, 9), (1, 9)), ((0, 9), (3, 9)))),
    ((2, 5), (((2, 5), (2, 7)), ((2, 5), (2, 6)))),
    ((0, 8), (((0, 8), (2, 8)), ((0, 8), (3, 8)), ((0, 8), (1, 8)))),
    ((0, 7), (((0, 7), (3, 7)), ((0, 7), (1, 7)))),
    ((3, 1), ()),
    ((1, 1), ()),
    ((1, 15), ()),
    ((3, 15), ()),
    ((2, 15), ()),
    ((1, 2), ()),
    ((3, 2), ()),
    ((1, 5), ()),
    ((3, 5), ()),
    ((3, 14), ()),
    ((2, 14), ()),
    ((1, 13), ()),
    ((2, 13), ()),
    ((2, 3), ()),
    ((0, 3), ()),
    ((3, 12), ()),
    ((1, 4), ()),
    ((2, 4), ()),
    ((3, 4), ()),
    ((1, 12), ()),
    ((3, 3), ()),
    ((0, 13), ()),
    ((1, 10), ()),
    ((3, 6), ()),
    ((1, 6), ()),
    ((3, 10), ()),
    ((2, 12), ()),
    ((2, 10), ()),
    ((0, 10), ()),
    ((1, 9), ()),
    ((3, 9), ()),
    ((3, 8), ()),
    ((1, 8), ()),
    ((2, 6), ()),
    ((3, 7), ()),
    ((2, 9), ()),
    ((1, 7), ()),
    ((2, 7), ()),
    ((2, 8), ()),
)


def kernel(
    tok_h, gain_h, wq_h, wo_h, gate_h, key_h, val_h, act_h, slot_h,
    out_ref,
    tbuf, abuf, wq, wo, gain, kbuf, vbuf, of, pbuf, gate_s, act_s, slot_s,
    local_sem, t_send, t_recv, a_send, a_recv, kv_send, kv_recv,
):
    dp = lax.axis_index("dp")
    mp = lax.axis_index("mp")
    y, z = dp // NZ, lax.rem(dp, NZ)
    x, core = mp // 2, lax.rem(mp, 2)
    ys = [lax.rem(y + d, NY) * NZ for d in range(NY)]
    zs = [lax.rem(z + d, NZ) for d in range(NZ)]
    xs = [lax.rem(x + d, NX) * 2 for d in range(NX)]

    def block(dy, dz):
        return ys[dy % NY] + zs[dz % NZ]

    def plane_peer(dy, dz):
        return (block(dy, dz), mp)

    def line_peer(px):
        return (dp, xs[px % NX] + core)

    sibling = (dp, xs[0] + (1 - core))

    local = [
        pltpu.make_async_copy(src, dst, local_sem.at[i])
        for i, (src, dst) in enumerate((
            (tok_h, tbuf.at[dp]),
            (gain_h, gain),
            (wq_h, wq),
            (wo_h, wo),
            (key_h, kbuf.at[pl.ds(mp * OWN, OWN)]),
            (val_h, vbuf.at[pl.ds(mp * OWN, OWN)]),
            (gate_h, gate_s),
            (act_h, act_s),
            (slot_h, slot_s),
        ))
    ]
    local[0].start()

    barrier = pltpu.get_barrier_semaphore()
    steps = {(a % NY, b % NZ) for _, (a, b) in NEAR_SPREAD[0][1]}
    steps |= {((-a) % NY, (-b) % NZ) for a, b in steps}
    partners = [plane_peer(*step) for step in sorted(steps)]
    partners += [line_peer(1), line_peer(-1), sibling]
    for peer in partners:
        pl.semaphore_signal(barrier, inc=1, device_id=peer, device_id_type=MESH)
    pl.semaphore_wait(barrier, len(partners))

    kv = ((kbuf, key_h), (vbuf, val_h))

    def images(px, same, part=None):
        first = (xs[px % NX] + (core if same else 1 - core)) * OWN
        if part is None:
            return pl.ds(pl.multiple_of(first, OWN), OWN)
        return pl.ds(pl.multiple_of(first + part * HALF, HALF), HALF)

    def kv_copy(which, source, where, peer, sem):
        return pltpu.make_async_remote_copy(
            src_ref=source, dst_ref=kv[which][0].at[where], send_sem=kv_send.at[which],
            recv_sem=kv_recv.at[which, sem], device_id=peer, device_id_type=MESH)

    ARRIVED = ((-1, 0), (-1, 1), (1, 0), (1, 1), (2, 0), (2, 1))

    def kv_own_half(which, px, part):
        source = kv[which][1].at[pl.ds(part * HALF, HALF)]
        kv_copy(which, source, images(0, True, part), line_peer(px), (0 if px == 1 else 2) + part).start()

    def kv_own_sibling(which):
        kv_copy(which, kv[which][1], images(0, True), sibling, 6).start()

    def kv_wait(which, where, sem):
        kv_copy(which, kv[which][0].at[where], where, sibling, sem).wait_recv()

    def kv_arrive(which, sem, onward=None):
        px, part = ARRIVED[sem]
        where = images(px, True, part)
        kv_wait(which, where, sem)
        source = kv[which][0].at[where]
        if onward is not None:
            kv_copy(which, source, where, line_peer(onward), 4 + part).start()
        kv_copy(which, source, where, sibling, 7 + sem).start()

    def kv_finish(which):
        kv_wait(which, images(0, False), 6)
        for sem, (px, part) in enumerate(ARRIVED):
            kv_wait(which, images(px, False, part), 7 + sem)

    def arrived_block(place):
        return block(-place[0], -place[1])

    def spread(tree, buf, send_sem, recv_sem, i):
        place, onward = tree[i]
        index_of = {node: k for k, (node, _) in enumerate(tree)}
        here = buf.at[arrived_block(place)]
        if i > 0:
            pltpu.make_async_remote_copy(
                src_ref=here, dst_ref=here, send_sem=send_sem, recv_sem=recv_sem.at[i],
                device_id=sibling, device_id_type=MESH).wait_recv()
        for origin, target in onward:
            here = buf.at[arrived_block(origin)]
            pltpu.make_async_remote_copy(
                src_ref=here, dst_ref=here, send_sem=send_sem, recv_sem=recv_sem.at[index_of[target]],
                device_id=plane_peer(target[0] - origin[0], target[1] - origin[1]),
                device_id_type=MESH).start()

    def all_sent(buf, send_sem):
        whole = buf.at[pl.ds(0, ND - 1)]
        pltpu.make_async_copy(whole, whole, send_sem).wait()

    for which, parts in ((0, (0, 1)), (1, (0,))):
        for part in parts:
            kv_own_half(which, 1, part)
            kv_own_half(which, -1, 1 - part)
        kv_own_sibling(which)
    local[0].wait()
    spread(NEAR_SPREAD, tbuf, t_send.at[0], t_recv, 0)
    for i in range(1, 9):
        local[i].start()

    own = tbuf[dp].astype(F32)
    shift = jnp.broadcast_to(jnp.sum(own, axis=1, keepdims=True) * (1.0 / DH), (ROWS, DH))
    total = own - shift
    square = total * total
    kv_steps = {
        5: ((0, 0, 1), (0, 3, -1)),
        15: ((0, 1, None), (0, 2, None)),
        25: ((1, 0, 1), (1, 3, -1)),
        50: ((0, 4, None), (0, 5, None)),
    }
    for i in range(1, ND):
        spread(NEAR_SPREAD, tbuf, t_send.at[0], t_recv, i)
        part = tbuf[arrived_block(NEAR_SPREAD[i][0])].astype(F32) - shift
        total = total + part
        square = square + part * part
        for which, sem, onward in kv_steps.get(i, ()):
            kv_arrive(which, sem, onward)
        if i == 5:
            kv_own_half(1, 1, 1)
            kv_own_half(1, -1, 0)

    drift = jnp.sum(total, axis=1, keepdims=True) * (1.0 / (ND * DH))
    variance = jnp.sum(square, axis=1, keepdims=True) * (1.0 / (ND * DH)) - drift * drift
    mean_b = shift + drift
    scale_b = jnp.broadcast_to(lax.rsqrt(jnp.maximum(variance, 0.0) + EPS), (ROWS, DH))
    local[1].wait()
    local[2].wait()

    def project(i, acc):
        parts = []
        for j in range(4):
            d = i * 4 + j
            g = gain[pl.ds(d, 1), :]
            parts.append((((tbuf[d].astype(F32) - mean_b) * scale_b) * g).astype(BF16))
        lhs = jnp.concatenate(parts, axis=1)
        rhs = wq[pl.ds(pl.multiple_of(i * 4 * DH, 4 * DH), 4 * DH), :]
        return acc + jnp.dot(lhs, rhs, preferred_element_type=F32)

    queries = lax.fori_loop(0, ND // 4, project, jnp.zeros((ROWS, DH), F32), unroll=4)
    queries_b = queries.astype(BF16)

    kv_arrive(1, 1)
    kv_arrive(1, 2)
    for i in (4, 7, 8):
        local[i].wait()
    kv_finish(0)

    def slot_of(i, j):
        image = act_s[j % 4, mp * (ROWS // 4) + i * 2 + j // 4]
        return slot_s[image]

    lane = lax.broadcasted_iota(jnp.int32, (VT, ROWS), 1)

    def score(i, acc):
        keys = jnp.concatenate([kbuf[slot_of(i, j)] for j in range(8)], axis=0)
        each = lax.dot_general(keys, queries_b, (((1,), (1,)), ((), ())), preferred_element_type=F32)
        for j in range(8):
            acc = jnp.where(lane == i * 8 + j, each[j * VT:(j + 1) * VT], acc)
        return acc

    s = lax.fori_loop(0, ROWS // 8, score, jnp.zeros((VT, ROWS), F32)) * (DH ** -0.5)
    e = jnp.exp(s - jnp.max(s, axis=0, keepdims=True))
    p = (e / jnp.sum(e, axis=0, keepdims=True)).astype(BF16).astype(F32)
    for r in range(ROWS):
        pbuf[r] = jnp.broadcast_to(p[:, r:r + 1], (VT, DH))

    kv_arrive(1, 4)
    kv_arrive(1, 5)
    local[5].wait()
    kv_finish(1)

    def collect(i, carry):
        outs = [
            jnp.sum(pbuf[i * 8 + j] * vbuf[slot_of(i, j)].astype(F32), axis=0, keepdims=True)
            for j in range(8)
        ]
        of[pl.ds(pl.multiple_of(i * 8, 8), 8), :] = jnp.concatenate(outs, axis=0)
        return carry

    lax.fori_loop(0, ROWS // 8, collect, 0)
    abuf[dp] = of[...].astype(BF16)

    final = max(i for i, (_, onward) in enumerate(FAR_SPREAD) if onward) + 1
    for i in range(final):
        spread(FAR_SPREAD, abuf, a_send.at[0], a_recv, i)
    local[3].wait()

    def project_out(acc, first, last):
        places = [arrived_block(FAR_SPREAD[i][0]) for i in range(first, last)]
        lhs = jnp.concatenate([abuf[b] for b in places], axis=1)
        rhs = jnp.concatenate([wo[pl.ds(pl.multiple_of(b * DH, DH), DH), :] for b in places], axis=0)
        return acc + jnp.dot(lhs, rhs, preferred_element_type=F32)

    projected = jnp.zeros((ROWS, DH), F32)
    for first in range(0, final, 8):
        projected = project_out(projected, first, min(first + 8, final))
    for first in range(final, ND, 4):
        last = min(first + 4, ND)
        for i in range(first, last):
            spread(FAR_SPREAD, abuf, a_send.at[0], a_recv, i)
        projected = project_out(projected, first, last)
    local[6].wait()
    gate = jnp.tanh(jnp.full((ROWS, DH), gate_s[0], F32))
    out_ref[...] = (tbuf[dp].astype(F32) + gate * projected).astype(BF16)

    all_sent(tbuf, t_send.at[0])
    all_sent(abuf, a_send.at[0])
    for which in (0, 1):
        whole = kv[which][0].at[pl.ds(0, 7 * OWN)]
        pltpu.make_async_copy(whole, whole, kv_send.at[which]).wait()


def body(tokens, norm_gain, query_weight, out_weight, gate_scalar, image_keys, image_values, active_image, image_slot):
    hbm = pl.BlockSpec(memory_space=pltpu.HBM)
    vmem = pl.BlockSpec(memory_space=pltpu.VMEM)
    dma = pltpu.SemaphoreType.DMA
    return pl.pallas_call(
        kernel,
        out_shape=pltpu.VMEM((ROWS, DH), BF16),
        in_specs=[hbm] * 9,
        out_specs=vmem,
        scratch_shapes=[
            pltpu.VMEM((ND, ROWS, DH), BF16),
            pltpu.VMEM((ND, ROWS, DH), BF16),
            pltpu.VMEM((ND * DH, DH), BF16),
            pltpu.VMEM((ND * DH, DH), BF16),
            pltpu.VMEM((ND, DH), F32),
            pltpu.VMEM((IMAGES, VT, DH), BF16),
            pltpu.VMEM((IMAGES, VT, DH), BF16),
            pltpu.VMEM((ROWS, DH), F32),
            pltpu.VMEM((ROWS, VT, DH), F32),
            pltpu.SMEM((1,), F32),
            pltpu.SMEM((4, 128), jnp.int32),
            pltpu.SMEM((IMAGES,), jnp.int32),
            dma((9,)),
            dma((1,)),
            dma((ND,)),
            dma((1,)),
            dma((ND,)),
            dma((2,)),
            dma((2, 13)),
        ],
        compiler_params=pltpu.CompilerParams(
            collective_id=0, has_side_effects=True, vmem_limit_bytes=56 * 1024 * 1024
        ),
        name="gated_cross_attention",
    )(tokens, norm_gain.reshape(ND, DH), query_weight, out_weight, gate_scalar,
      image_keys, image_values, active_image.T, image_slot)


def solution(mesh):
    placed = (
        P("mp", "dp"),
        P(),
        P(None, "dp"),
        P(None, "dp"),
        P(),
        P("mp", None, "dp"),
        P("mp", None, "dp"),
        P(),
        P(),
    )
    return jax.shard_map(body, mesh=mesh, in_specs=placed, out_specs=P("mp", "dp"), check_vma=False)
```

```python
import jax
import jax.numpy as jnp
from jax import lax
from jax.experimental import pallas as pl
from jax.experimental.pallas import tpu as pltpu
from jax.sharding import PartitionSpec as P

MESH = pl.DeviceIdType.MESH
NY, NZ, NX = 4, 16, 4
ND = NY * NZ
ROWS = 64
DH = 128
VT = 64
OWN = 16
HALF = OWN // 2
IMAGES = 128
EPS = 1e-05
F32 = jnp.float32
BF16 = jnp.bfloat16

NEAR_SPREAD = (
    ((0, 0), (((0, 0), (0, 14)), ((0, 0), (1, 0)), ((0, 0), (0, 2)), ((0, 0), (3, 0)), ((0, 0), (0, 1)))),
    ((1, 0), (((1, 0), (1, 1)),)),
    ((3, 0), (((3, 0), (2, 0)), ((3, 0), (3, 15)), ((3, 0), (3, 1)))),
    ((0, 14), (((0, 14), (3, 14)), ((0, 14), (1, 14)))),
    ((0, 2), (((0, 14), (0, 10)), ((0, 2), (0, 6)), ((0, 2), (0, 4)), ((0, 2), (2, 2)), ((0, 2), (3, 2)), ((0, 2), (1, 2)))),
    ((1, 1), (((1, 1), (2, 1)),)),
    ((3, 15), (((3, 15), (1, 15)), ((3, 15), (0, 15)), ((3, 15), (2, 15)))),
    ((3, 1), (((3, 1), (3, 3)),)),
    ((3, 14), (((3, 14), (3, 12)), ((3, 14), (3, 13)))),
    ((1, 14), (((1, 14), (2, 14)), ((1, 14), (1, 13)))),
    ((1, 2), (((1, 2), (1, 3)),)),
    ((2, 2), (((2, 2), (2, 3)),)),
    ((0, 4), (((0, 4), (0, 5)), ((0, 4), (3, 4)), ((0, 4), (1, 4)), ((0, 4), (0, 3)))),
    ((0, 10), (((0, 10), (0, 8)), ((0, 10), (3, 10)), ((0, 10), (1, 10)), ((0, 10), (0, 11)), ((0, 10), (2, 10)))),
    ((0, 6), (((0, 6), (0, 7)), ((0, 6), (0, 9)), ((0, 6), (2, 6)), ((0, 6), (3, 6)), ((0, 6), (1, 6)))),
    ((2, 15), (((2, 15), (2, 13)),)),
    ((2, 14), (((2, 14), (2, 11)),)),
    ((1, 13), (((1, 13), (0, 13)), ((1, 13), (1, 12)))),
    ((2, 3), (((2, 3), (2, 5)),)),
    ((3, 12), (((3, 12), (0, 12)), ((3, 12), (2, 12)))),
    ((3, 4), (((3, 4), (2, 4)),)),
    ((0, 5), (((0, 5), (1, 5)), ((0, 5), (3, 5)))),
    ((3, 10), (((3, 10), (3, 11)), ((3, 10), (3, 9)))),
    ((1, 10), (((1, 10), (1, 9)),)),
    ((0, 11), (((0, 11), (1, 11)),)),
    ((0, 7), (((0, 7), (3, 7)),)),
    ((0, 8), (((0, 8), (2, 8)), ((0, 8), (1, 8)), ((0, 8), (3, 8)))),
    ((1, 6), (((1, 6), (1, 7)),)),
    ((2, 10), (((2, 10), (2, 9)),)),
    ((2, 6), (((2, 6), (2, 7)),)),
    ((0, 1), ()),
    ((2, 0), ()),
    ((3, 2), ()),
    ((2, 1), ()),
    ((0, 15), ()),
    ((1, 15), ()),
    ((3, 3), ()),
    ((3, 13), ()),
    ((1, 3), ()),
    ((1, 4), ()),
    ((0, 3), ()),
    ((3, 6), ()),
    ((2, 13), ()),
    ((0, 13), ()),
    ((0, 9), ()),
    ((1, 12), ()),
    ((0, 12), ()),
    ((2, 12), ()),
    ((1, 5), ()),
    ((2, 4), ()),
    ((3, 11), ()),
    ((3, 9), ()),
    ((3, 5), ()),
    ((1, 11), ()),
    ((2, 5), ()),
    ((2, 11), ()),
    ((3, 7), ()),
    ((1, 9), ()),
    ((1, 7), ()),
    ((3, 8), ()),
    ((1, 8), ()),
    ((2, 9), ()),
    ((2, 7), ()),
    ((2, 8), ()),
)
FAR_SPREAD = (
    ((0, 0), (((0, 0), (0, 11)), ((0, 0), (3, 0)), ((0, 0), (2, 0)), ((0, 0), (0, 1)), ((0, 0), (0, 15)), ((0, 0), (0, 5)), ((0, 0), (0, 2)), ((0, 0), (1, 0)))),
    ((3, 0), (((3, 0), (3, 13)),)),
    ((0, 1), (((0, 1), (3, 1)), ((0, 1), (1, 1)))),
    ((0, 15), (((0, 15), (2, 15)), ((0, 15), (0, 14)), ((0, 15), (3, 15)), ((0, 15), (1, 15)))),
    ((1, 0), (((1, 0), (1, 3)), ((1, 0), (1, 14)))),
    ((2, 0), (((2, 0), (2, 1)),)),
    ((0, 2), (((0, 2), (2, 2)), ((0, 2), (0, 4)), ((0, 2), (3, 2)), ((0, 2), (1, 2)))),
    ((0, 11), (((0, 11), (0, 8)), ((0, 11), (2, 11)), ((0, 11), (3, 11)), ((0, 11), (1, 11)), ((0, 11), (0, 9)), ((0, 11), (0, 12)))),
    ((0, 5), (((0, 5), (2, 5)), ((0, 5), (1, 5)), ((0, 5), (0, 6)), ((0, 5), (3, 5)), ((0, 5), (0, 7)))),
    ((0, 14), (((0, 14), (3, 14)),)),
    ((2, 1), (((2, 1), (2, 4)),)),
    ((1, 14), (((1, 14), (2, 14)), ((1, 14), (1, 13)), ((1, 14), (1, 12)))),
    ((3, 13), (((3, 13), (2, 13)), ((3, 13), (3, 12)))),
    ((1, 3), (((1, 3), (3, 3)), ((1, 3), (0, 3)))),
    ((2, 2), (((2, 2), (2, 3)),)),
    ((0, 4), (((0, 4), (1, 4)), ((0, 4), (3, 4)))),
    ((1, 11), (((1, 11), (1, 10)),)),
    ((0, 12), (((0, 12), (0, 13)),)),
    ((3, 11), (((3, 11), (3, 10)),)),
    ((0, 6), (((0, 6), (3, 6)), ((0, 6), (1, 6)))),
    ((2, 11), (((2, 11), (2, 12)), ((2, 11), (2, 10)), ((2, 11), (2, 9)))),
    ((0, 9), (((0, 9), (0, 10)), ((0, 9), (1, 9)), ((0, 9), (3, 9)))),
    ((2, 5), (((2, 5), (2, 7)), ((2, 5), (2, 6)))),
    ((0, 8), (((0, 8), (2, 8)), ((0, 8), (3, 8)), ((0, 8), (1, 8)))),
    ((0, 7), (((0, 7), (3, 7)), ((0, 7), (1, 7)))),
    ((3, 1), ()),
    ((1, 1), ()),
    ((1, 15), ()),
    ((3, 15), ()),
    ((2, 15), ()),
    ((1, 2), ()),
    ((3, 2), ()),
    ((1, 5), ()),
    ((3, 5), ()),
    ((3, 14), ()),
    ((2, 14), ()),
    ((1, 13), ()),
    ((2, 13), ()),
    ((2, 3), ()),
    ((0, 3), ()),
    ((3, 12), ()),
    ((1, 4), ()),
    ((2, 4), ()),
    ((3, 4), ()),
    ((1, 12), ()),
    ((3, 3), ()),
    ((0, 13), ()),
    ((1, 10), ()),
    ((3, 6), ()),
    ((1, 6), ()),
    ((3, 10), ()),
    ((2, 12), ()),
    ((2, 10), ()),
    ((0, 10), ()),
    ((1, 9), ()),
    ((3, 9), ()),
    ((3, 8), ()),
    ((1, 8), ()),
    ((2, 6), ()),
    ((3, 7), ()),
    ((2, 9), ()),
    ((1, 7), ()),
    ((2, 7), ()),
    ((2, 8), ()),
)


def kernel(
    tok_h, gain_h, wq_h, wo_h, gate_h, key_h, val_h, act_h, slot_h,
    out_ref,
    tbuf, abuf, wq, wo, gain, kbuf, vbuf, of, pbuf, gate_s, act_s, slot_s,
    local_sem, t_send, t_recv, a_send, a_recv, kv_send, kv_recv,
):
    dp = lax.axis_index("dp")
    mp = lax.axis_index("mp")
    y, z = dp // NZ, lax.rem(dp, NZ)
    x, core = mp // 2, lax.rem(mp, 2)
    ys = [lax.rem(y + d, NY) * NZ for d in range(NY)]
    zs = [lax.rem(z + d, NZ) for d in range(NZ)]
    xs = [lax.rem(x + d, NX) * 2 for d in range(NX)]

    def block(dy, dz):
        return ys[dy % NY] + zs[dz % NZ]

    def plane_peer(dy, dz):
        return (block(dy, dz), mp)

    def line_peer(px):
        return (dp, xs[px % NX] + core)

    sibling = (dp, xs[0] + (1 - core))

    local = [
        pltpu.make_async_copy(src, dst, local_sem.at[i])
        for i, (src, dst) in enumerate((
            (tok_h, tbuf.at[dp]),
            (gain_h, gain),
            (wq_h, wq),
            (wo_h, wo),
            (key_h, kbuf.at[pl.ds(mp * OWN, OWN)]),
            (val_h, vbuf.at[pl.ds(mp * OWN, OWN)]),
            (gate_h, gate_s),
            (act_h, act_s),
            (slot_h, slot_s),
        ))
    ]
    local[0].start()

    barrier = pltpu.get_barrier_semaphore()
    steps = {(a % NY, b % NZ) for _, (a, b) in NEAR_SPREAD[0][1]}
    steps |= {((-a) % NY, (-b) % NZ) for a, b in steps}
    partners = [plane_peer(*step) for step in sorted(steps)]
    partners += [line_peer(1), line_peer(-1), sibling]
    for peer in partners:
        pl.semaphore_signal(barrier, inc=1, device_id=peer, device_id_type=MESH)
    pl.semaphore_wait(barrier, len(partners))

    kv = ((kbuf, key_h), (vbuf, val_h))

    def images(px, same, part=None):
        first = (xs[px % NX] + (core if same else 1 - core)) * OWN
        if part is None:
            return pl.ds(pl.multiple_of(first, OWN), OWN)
        return pl.ds(pl.multiple_of(first + part * HALF, HALF), HALF)

    def kv_copy(which, source, where, peer, sem):
        return pltpu.make_async_remote_copy(
            src_ref=source, dst_ref=kv[which][0].at[where], send_sem=kv_send.at[which],
            recv_sem=kv_recv.at[which, sem], device_id=peer, device_id_type=MESH)

    ARRIVED = ((-1, 0), (-1, 1), (1, 0), (1, 1), (2, 0), (2, 1))

    def kv_own_half(which, px, part):
        source = kv[which][1].at[pl.ds(part * HALF, HALF)]
        kv_copy(which, source, images(0, True, part), line_peer(px), (0 if px == 1 else 2) + part).start()

    def kv_own_sibling(which):
        kv_copy(which, kv[which][1], images(0, True), sibling, 6).start()

    def kv_wait(which, where, sem):
        kv_copy(which, kv[which][0].at[where], where, sibling, sem).wait_recv()

    def kv_arrive(which, sem, onward=None):
        px, part = ARRIVED[sem]
        where = images(px, True, part)
        kv_wait(which, where, sem)
        source = kv[which][0].at[where]
        if onward is not None:
            kv_copy(which, source, where, line_peer(onward), 4 + part).start()
        kv_copy(which, source, where, sibling, 7 + sem).start()

    def kv_finish(which):
        kv_wait(which, images(0, False), 6)
        for sem, (px, part) in enumerate(ARRIVED):
            kv_wait(which, images(px, False, part), 7 + sem)

    def arrived_block(place):
        return block(-place[0], -place[1])

    def spread(tree, buf, send_sem, recv_sem, i):
        place, onward = tree[i]
        index_of = {node: k for k, (node, _) in enumerate(tree)}
        here = buf.at[arrived_block(place)]
        if i > 0:
            pltpu.make_async_remote_copy(
                src_ref=here, dst_ref=here, send_sem=send_sem, recv_sem=recv_sem.at[i],
                device_id=sibling, device_id_type=MESH).wait_recv()
        for origin, target in onward:
            here = buf.at[arrived_block(origin)]
            pltpu.make_async_remote_copy(
                src_ref=here, dst_ref=here, send_sem=send_sem, recv_sem=recv_sem.at[index_of[target]],
                device_id=plane_peer(target[0] - origin[0], target[1] - origin[1]),
                device_id_type=MESH).start()

    def all_sent(buf, send_sem):
        whole = buf.at[pl.ds(0, ND - 1)]
        pltpu.make_async_copy(whole, whole, send_sem).wait()

    for which, parts in ((0, (0, 1)), (1, (0,))):
        for part in parts:
            kv_own_half(which, 1, part)
            kv_own_half(which, -1, 1 - part)
        kv_own_sibling(which)
    local[0].wait()
    spread(NEAR_SPREAD, tbuf, t_send.at[0], t_recv, 0)
    for i in range(1, 9):
        local[i].start()

    own = tbuf[dp].astype(F32)
    shift = jnp.broadcast_to(jnp.sum(own, axis=1, keepdims=True) * (1.0 / DH), (ROWS, DH))
    total = own - shift
    square = total * total
    kv_steps = {
        5: ((0, 0, 1), (0, 3, -1)),
        15: ((0, 1, None), (0, 2, None)),
        25: ((1, 0, 1), (1, 3, -1)),
        50: ((0, 4, None), (0, 5, None)),
    }
    for i in range(1, ND):
        spread(NEAR_SPREAD, tbuf, t_send.at[0], t_recv, i)
        part = tbuf[arrived_block(NEAR_SPREAD[i][0])].astype(F32) - shift
        total = total + part
        square = square + part * part
        for which, sem, onward in kv_steps.get(i, ()):
            kv_arrive(which, sem, onward)
        if i == 5:
            kv_own_half(1, 1, 1)
            kv_own_half(1, -1, 0)

    drift = jnp.sum(total, axis=1, keepdims=True) * (1.0 / (ND * DH))
    variance = jnp.sum(square, axis=1, keepdims=True) * (1.0 / (ND * DH)) - drift * drift
    mean_b = shift + drift
    scale_b = jnp.broadcast_to(lax.rsqrt(jnp.maximum(variance, 0.0) + EPS), (ROWS, DH))
    local[1].wait()
    local[2].wait()

    def project(i, acc):
        parts = []
        for j in range(4):
            d = i * 4 + j
            g = gain[pl.ds(d, 1), :]
            parts.append((((tbuf[d].astype(F32) - mean_b) * scale_b) * g).astype(BF16))
        lhs = jnp.concatenate(parts, axis=1)
        rhs = wq[pl.ds(pl.multiple_of(i * 4 * DH, 4 * DH), 4 * DH), :]
        return acc + jnp.dot(lhs, rhs, preferred_element_type=F32)

    queries = lax.fori_loop(0, ND // 4, project, jnp.zeros((ROWS, DH), F32), unroll=4)
    queries_b = queries.astype(BF16)

    kv_arrive(1, 1)
    kv_arrive(1, 2)
    for i in (4, 7, 8):
        local[i].wait()
    kv_finish(0)

    def slot_of(i, j):
        image = act_s[j % 4, mp * (ROWS // 4) + i * 2 + j // 4]
        return slot_s[image]

    lane = lax.broadcasted_iota(jnp.int32, (VT, ROWS), 1)

    def score(i, acc):
        keys = jnp.concatenate([kbuf[slot_of(i, j)] for j in range(8)], axis=0)
        each = lax.dot_general(keys, queries_b, (((1,), (1,)), ((), ())), preferred_element_type=F32)
        for j in range(8):
            acc = jnp.where(lane == i * 8 + j, each[j * VT:(j + 1) * VT], acc)
        return acc

    s = lax.fori_loop(0, ROWS // 8, score, jnp.zeros((VT, ROWS), F32)) * (DH ** -0.5)
    e = jnp.exp(s - jnp.max(s, axis=0, keepdims=True))
    p = (e / jnp.sum(e, axis=0, keepdims=True)).astype(BF16).astype(F32)
    for r in range(ROWS):
        pbuf[r] = jnp.broadcast_to(p[:, r:r + 1], (VT, DH))

    kv_arrive(1, 4)
    kv_arrive(1, 5)
    local[5].wait()
    kv_finish(1)

    def collect(i, carry):
        outs = [
            jnp.sum(pbuf[i * 8 + j] * vbuf[slot_of(i, j)].astype(F32), axis=0, keepdims=True)
            for j in range(8)
        ]
        of[pl.ds(pl.multiple_of(i * 8, 8), 8), :] = jnp.concatenate(outs, axis=0)
        return carry

    lax.fori_loop(0, ROWS // 8, collect, 0)
    abuf[dp] = of[...].astype(BF16)

    final = max(i for i, (_, onward) in enumerate(FAR_SPREAD) if onward) + 1
    for i in range(final):
        spread(FAR_SPREAD, abuf, a_send.at[0], a_recv, i)
    local[3].wait()

    def project_out(acc, first, last):
        places = [arrived_block(FAR_SPREAD[i][0]) for i in range(first, last)]
        lhs = jnp.concatenate([abuf[b] for b in places], axis=1)
        rhs = jnp.concatenate([wo[pl.ds(pl.multiple_of(b * DH, DH), DH), :] for b in places], axis=0)
        return acc + jnp.dot(lhs, rhs, preferred_element_type=F32)

    projected = jnp.zeros((ROWS, DH), F32)
    for first in range(0, final, 8):
        projected = project_out(projected, first, min(first + 8, final))
    local[6].wait()
    gate = jnp.tanh(jnp.full((ROWS, DH), gate_s[0], F32))
    cuts = [*range(final, ND - 2, 6), ND - 2, ND]
    for first, last in zip(cuts, cuts[1:]):
        for i in range(first, last):
            spread(FAR_SPREAD, abuf, a_send.at[0], a_recv, i)
        projected = project_out(projected, first, last)
    out_ref[...] = (tbuf[dp].astype(F32) + gate * projected).astype(BF16)

    all_sent(tbuf, t_send.at[0])
    all_sent(abuf, a_send.at[0])
    for which in (0, 1):
        whole = kv[which][0].at[pl.ds(0, 7 * OWN)]
        pltpu.make_async_copy(whole, whole, kv_send.at[which]).wait()


def body(tokens, norm_gain, query_weight, out_weight, gate_scalar, image_keys, image_values, active_image, image_slot):
    hbm = pl.BlockSpec(memory_space=pltpu.HBM)
    vmem = pl.BlockSpec(memory_space=pltpu.VMEM)
    dma = pltpu.SemaphoreType.DMA
    return pl.pallas_call(
        kernel,
        out_shape=pltpu.VMEM((ROWS, DH), BF16),
        in_specs=[hbm] * 9,
        out_specs=vmem,
        scratch_shapes=[
            pltpu.VMEM((ND, ROWS, DH), BF16),
            pltpu.VMEM((ND, ROWS, DH), BF16),
            pltpu.VMEM((ND * DH, DH), BF16),
            pltpu.VMEM((ND * DH, DH), BF16),
            pltpu.VMEM((ND, DH), F32),
            pltpu.VMEM((IMAGES, VT, DH), BF16),
            pltpu.VMEM((IMAGES, VT, DH), BF16),
            pltpu.VMEM((ROWS, DH), F32),
            pltpu.VMEM((ROWS, VT, DH), F32),
            pltpu.SMEM((1,), F32),
            pltpu.SMEM((4, 128), jnp.int32),
            pltpu.SMEM((IMAGES,), jnp.int32),
            dma((9,)),
            dma((1,)),
            dma((ND,)),
            dma((1,)),
            dma((ND,)),
            dma((2,)),
            dma((2, 13)),
        ],
        compiler_params=pltpu.CompilerParams(
            collective_id=0, has_side_effects=True, vmem_limit_bytes=56 * 1024 * 1024
        ),
        name="gated_cross_attention",
    )(tokens, norm_gain.reshape(ND, DH), query_weight, out_weight, gate_scalar,
      image_keys, image_values, active_image.T, image_slot)


def solution(mesh):
    placed = (
        P("mp", "dp"),
        P(),
        P(None, "dp"),
        P(None, "dp"),
        P(),
        P("mp", None, "dp"),
        P("mp", None, "dp"),
        P(),
        P(),
    )
    return jax.shard_map(body, mesh=mesh, in_specs=placed, out_specs=P("mp", "dp"), check_vma=False)
```
